256 devices in a mesh: parts: 4 (over y, x), ka: 64 (over z, core).
Axes of the slice: x: 2, y: 2, z: 32, core: 2. Of those that a mesh axis runs over, the one named last changes fastest.
The devices are a block of a 4x8x32 slice.
Arguments:
- energies: float32 [256, 200], P(('parts', 'ka')), parts along dimension 0, may hold values from -4 to 4
- proj: float32 [256, 2, 10, 200], P(('parts', 'ka')), parts along dimension 0, may hold values from -0.3125 to 0.3125
- window: int32 [256, 2], P(('parts', 'ka')), parts along dimension 0, may hold values from 0 to 200, as said below
- sigma: float32 [8, 10, 10, 256], P('parts', None, None, 'ka'), parts along dimension 0, may hold values from -3 to 1.5, as said below
- impurity_inverse: float32 [8, 10, 10, 256], P('parts', None, None, 'ka'), parts along dimension 0, may hold values from -5 to 50, as said below
Outputs:
- density: float32 [256, 2, 200, 200], P(('parts', 'ka')), parts along dimension 0
- sigma_new: float32 [8, 10, 10, 256], P('parts', None, None, 'ka'), parts along dimension 0
The draws below stay inside these ranges and needn't reach their ends.
There are 4 independent parts, one for each index of `parts`. The reference program is written for one: setup_inputs(seed, part) draws one part's arguments, and reference() takes and returns one part's arrays. A program takes and returns all parts, laid end to end along the dimension named above; each array names one. Nothing has to cross between parts.
Inputs may be any that keep to these rules, and one draw needn't show every extreme that they name: window[k, 0] < 40 and window[k, 1] >= 160 for every k-point. For every frequency, sigma[0] and sigma[1] are real symmetric matrices and -sigma[1] is positive definite with smallest eigenvalue 0.2 or more. For every frequency n, impurity_inverse[0] and impurity_inverse[1] are real symmetric matrices and impurity_inverse[1] + sigma[1] - freqs[n] times the identity is positive definite with smallest eigenvalue 0.2 or more.
All inputs are finite; a program needn't handle non-finite values.
Results may differ from the reference program's by a relative error of at most 0.00011.
Values sent between devices are 32-bit elements; how exact they have to be, the bound alone decides.
No kernel may reach another device: no remote copies, remote signals or barrier semaphores. Data moves between devices by JAX's collectives and lax.ppermute only.
A program may use at most 64 MiB of HBM per device.

```python
import math
import jax
import jax.numpy as jnp
from jax import lax

NORB = 10
NB = 200
NW = 256
K = 64


def draw_window(key, part):
    first = jax.random.randint(jax.random.fold_in(key, 11), (K,), 0, NB // 5)
    last = jax.random.randint(jax.random.fold_in(key, 12), (K,), NB - NB // 5, NB + 1)
    return jnp.stack([first, last], axis=1).astype(jnp.int32)


def sigma_parts(key):
    hermit = jnp.clip(0.5 * jax.random.normal(jax.random.fold_in(key, 21), (NORB, NORB, NW), jnp.float32), -1.5, 1.5)
    hermit = 0.5 * (hermit + jnp.swapaxes(hermit, 0, 1))
    damping = jnp.exp(jax.random.uniform(jax.random.fold_in(key, 22), (NORB, NW), jnp.float32, jnp.log(0.3), jnp.log(3.0)))
    offdiag = jax.random.uniform(jax.random.fold_in(key, 23), (NORB, NORB, NW), jnp.float32, -0.01, 0.01)
    ident = jnp.eye(NORB, dtype=jnp.float32)[:, :, None]
    offdiag = 0.5 * (offdiag + jnp.swapaxes(offdiag, 0, 1)) * (1.0 - ident)
    gamma = offdiag + ident * damping[:, None, :]
    return (hermit, gamma)


def draw_sigma(key, part):
    hermit, gamma = sigma_parts(key)
    return jnp.stack([hermit, -gamma]).astype(jnp.float32)


def draw_impurity_inverse(key, part):
    hermit, gamma = sigma_parts(key)
    level = jnp.clip(0.4 * jax.random.normal(jax.random.fold_in(key, 31), (NORB, NORB, NW), jnp.float32), -1.0, 1.0)
    level = 0.5 * (level + jnp.swapaxes(level, 0, 1))
    factor = jnp.clip(jax.random.normal(jax.random.fold_in(key, 32), (NORB, NORB, NW), jnp.float32), -3.0, 3.0)
    ident = jnp.eye(NORB, dtype=jnp.float32)[:, :, None]
    bath = 0.5 * jnp.einsum('ikn,jkn->ijn', factor, factor) / NORB + 0.2 * ident
    freqs = (2.0 * jnp.arange(NW).astype(jnp.float32) + 1.0) * (math.pi / 40.0)
    imag = ident * freqs[None, None, :] + bath + gamma
    return jnp.stack([level, imag]).astype(jnp.float32)


def steps_of(stream_key, dims, cuts, smallest, largest):
    def one(dim, parts):
        heights = jax.random.uniform(jax.random.fold_in(jax.random.fold_in(stream_key, 6), dim), (parts,), jnp.float32, smallest / len(cuts), largest / len(cuts))
        return jnp.repeat(jnp.exp(heights), dims[dim] // parts).reshape((-1,) + (1,) * (len(dims) - dim - 1))

    gain = one(*cuts[0])
    for cut in cuts[1:]:
        gain = gain * one(*cut)
    return gain


def noise(key, shape, deviation, most, pieces=(), held_as=jnp.bfloat16):
    gain = steps_of(key, shape, pieces, -0.22, 0.18) if pieces else 1.0
    entries = jax.random.normal(key, shape, jnp.float32) * deviation * gain
    return jnp.minimum(jnp.maximum(entries, -most), most).astype(held_as)


def setup_inputs(seed: int = 0, part: int = 0) -> dict:
    key_of = jax.random.split(jax.random.key(seed), 6)
    part_keys = jax.random.split(jax.random.fold_in(key_of[5], part), 6)
    return {
        "energies": jnp.clip(jax.random.uniform(part_keys[0], (K, NB), jnp.float32, -4.0, 4.0) * steps_of(part_keys[0], (K, NB), ((0, 64),), -0.4, 0.0), -4.0, 4.0),
        "proj": noise(part_keys[1], (K, 2, NORB, NB), (2 * NB) ** -0.5, 0.3125, ((0, 64),), jnp.float32),
        "window": draw_window(jax.random.fold_in(jax.random.fold_in(key_of[5], part), 71), part),
        "sigma": draw_sigma(jax.random.fold_in(jax.random.fold_in(key_of[5], part), 71), part),
        "impurity_inverse": draw_impurity_inverse(jax.random.fold_in(jax.random.fold_in(key_of[5], part), 71), part),
    }


highest = lax.Precision.HIGHEST
inverse_temp = 40.0


def matsubara(first, count):
    return (2.0 * (first + jnp.arange(count)).astype(jnp.float32) + 1.0) * (math.pi / inverse_temp)


def tail_weight(count):
    total = 0.0
    for number in range(count):
        total += (inverse_temp / (math.pi * (2 * number + 1))) ** 2
    return inverse_temp / 4.0 - 2.0 / inverse_temp * total


def propagators(energy, freqs):
    energy_b = energy[:, None, :]
    freq_b = freqs[None, :, None]
    denom = energy_b * energy_b + freq_b * freq_b
    return -energy_b / denom, -freq_b / denom


def hybrid(proj, green_re, green_im):
    proj_re = proj[:, 0]
    proj_im = proj[:, 1]
    left_re = proj_re[:, None] * green_re[:, :, None] - proj_im[:, None] * green_im[:, :, None]
    left_im = proj_re[:, None] * green_im[:, :, None] + proj_im[:, None] * green_re[:, :, None]
    hyb_re = jnp.einsum('kwib,kjb->ijkw', left_re, proj_re, precision=highest) + jnp.einsum('kwib,kjb->ijkw', left_im, proj_im, precision=highest)
    hyb_im = jnp.einsum('kwib,kjb->ijkw', left_im, proj_re, precision=highest) - jnp.einsum('kwib,kjb->ijkw', left_re, proj_im, precision=highest)
    return hyb_re, hyb_im


def invert(mat_re, mat_im):
    size = mat_re.shape[0]
    ident = jnp.eye(size, dtype=jnp.float32).reshape((size, size) + (1,) * (mat_re.ndim - 2)) * jnp.ones_like(mat_re)
    aug_re = jnp.concatenate([mat_re, ident], axis=1)
    aug_im = jnp.concatenate([mat_im, jnp.zeros_like(ident)], axis=1)
    for pivot in range(size):
        piv_re = aug_re[pivot, pivot]
        piv_im = aug_im[pivot, pivot]
        denom = piv_re * piv_re + piv_im * piv_im
        rec_re = piv_re / denom
        rec_im = -piv_im / denom
        row_re = aug_re[pivot] * rec_re - aug_im[pivot] * rec_im
        row_im = aug_re[pivot] * rec_im + aug_im[pivot] * rec_re
        col_re = aug_re[:, pivot][:, None]
        col_im = aug_im[:, pivot][:, None]
        next_re = aug_re - (col_re * row_re[None] - col_im * row_im[None])
        next_im = aug_im - (col_re * row_im[None] + col_im * row_re[None])
        aug_re = next_re.at[pivot].set(row_re)
        aug_im = next_im.at[pivot].set(row_im)
    return aug_re[:, size:], aug_im[:, size:]


def cmul(first_re, first_im, second_re, second_im):
    out_re = jnp.einsum('ij...,jk...->ik...', first_re, second_re, precision=highest) - jnp.einsum('ij...,jk...->ik...', first_im, second_im, precision=highest)
    out_im = jnp.einsum('ij...,jk...->ik...', first_re, second_im, precision=highest) + jnp.einsum('ij...,jk...->ik...', first_im, second_re, precision=highest)
    return out_re, out_im


def update_sigma(sig_re, sig_im, loc_re, loc_im, imp_re, imp_im):
    inv_re, inv_im = invert(loc_re, loc_im)
    diff_re = inv_re - imp_re
    diff_im = inv_im - imp_im
    new_re = sig_re + 0.5 * (diff_re + jnp.swapaxes(diff_re, 0, 1))
    new_im = sig_im + 0.5 * (diff_im - jnp.swapaxes(diff_im, 0, 1))
    return new_re, new_im


def dressed(ainv_re, ainv_im, sig_re, sig_im):
    return invert(ainv_re - sig_re[:, :, None, :], ainv_im - sig_im[:, :, None, :])


def vertex(sig_re, sig_im, gorb_re, gorb_im):
    wide_re = jnp.broadcast_to(sig_re[:, :, None, :], gorb_re.shape)
    wide_im = jnp.broadcast_to(sig_im[:, :, None, :], gorb_im.shape)
    half_re, half_im = cmul(wide_re, wide_im, gorb_re, gorb_im)
    full_re, full_im = cmul(half_re, half_im, wide_re, wide_im)
    return wide_re + full_re, wide_im + full_im


def band_density_total(proj, green_re, green_im, vertex_real, vert_im):
    proj_re = proj[:, 0]
    proj_im = proj[:, 1]
    wide_gre = green_re[:, :, None, :]
    wide_gim = green_im[:, :, None, :]
    left_re = wide_gre * proj_re[:, None] + wide_gim * proj_im[:, None]
    left_im = wide_gim * proj_re[:, None] - wide_gre * proj_im[:, None]
    mixed_re = jnp.einsum('ijkw,kjb->kwib', vertex_real, proj_re, precision=highest) - jnp.einsum('ijkw,kjb->kwib', vert_im, proj_im, precision=highest)
    mixed_im = jnp.einsum('ijkw,kjb->kwib', vertex_real, proj_im, precision=highest) + jnp.einsum('ijkw,kjb->kwib', vert_im, proj_re, precision=highest)
    right_re = mixed_re * wide_gre - mixed_im * wide_gim
    right_im = mixed_re * wide_gim + mixed_im * wide_gre
    real_total = jnp.einsum('kwib,kwic->kbc', left_re, right_re, precision=highest) - jnp.einsum('kwib,kwic->kbc', left_im, right_im, precision=highest)
    imaginary_total = jnp.einsum('kwib,kwic->kbc', left_re, right_im, precision=highest) + jnp.einsum('kwib,kwic->kbc', left_im, right_re, precision=highest)
    return real_total, imaginary_total


def limit_term(proj, herm_re, herm_im):
    proj_re = proj[:, 0]
    proj_im = proj[:, 1]
    hp_re = jnp.einsum('ij,kjc->kic', herm_re, proj_re, precision=highest) - jnp.einsum('ij,kjc->kic', herm_im, proj_im, precision=highest)
    hp_im = jnp.einsum('ij,kjc->kic', herm_re, proj_im, precision=highest) + jnp.einsum('ij,kjc->kic', herm_im, proj_re, precision=highest)
    quad_re = jnp.einsum('kib,kic->kbc', proj_re, hp_re, precision=highest) + jnp.einsum('kib,kic->kbc', proj_im, hp_im, precision=highest)
    quad_im = jnp.einsum('kib,kic->kbc', proj_re, hp_im, precision=highest) - jnp.einsum('kib,kic->kbc', proj_im, hp_re, precision=highest)
    return quad_re, quad_im


def high_part(new_re, new_im):
    last_re = new_re[:, :, -1]
    last_im = new_im[:, :, -1]
    return 0.5 * (last_re + last_re.T), 0.5 * (last_im - last_im.T)


def reference(energies, proj, window, sigma, impurity_inverse):
    band = jnp.arange(NB, dtype=jnp.int32)
    inside = ((band[None, :] >= window[:, 0:1]) & (band[None, :] < window[:, 1:2])).astype(jnp.float32)
    masked_values = proj * inside[:, None, None, :]
    freqs = matsubara(0, NW)
    green_re, green_im = propagators(energies, freqs)
    hyb_re, hyb_im = hybrid(masked_values, green_re, green_im)
    ainv_re, ainv_im = invert(hyb_re, hyb_im)
    gorb_re, gorb_im = dressed(ainv_re, ainv_im, sigma[0], sigma[1])
    loc_re = jnp.sum(gorb_re, axis=2) / K
    loc_im = jnp.sum(gorb_im, axis=2) / K
    new_re, new_im = update_sigma(sigma[0], sigma[1], loc_re, loc_im, impurity_inverse[0], impurity_inverse[1])
    gnew_re, gnew_im = dressed(ainv_re, ainv_im, new_re, new_im)
    vertex_real, vert_im = vertex(new_re, new_im, gnew_re, gnew_im)

    def one_point(entry_list):
        kpoint_projector, kpoint_green_real, kpoint_green_imag, kpoint_vertex_real, kpoint_vertex_imag = entry_list
        real_total, imaginary_total = band_density_total(kpoint_projector[None], kpoint_green_real[None], kpoint_green_imag[None], kpoint_vertex_real[:, :, None, :], kpoint_vertex_imag[:, :, None, :])
        return real_total[0], imaginary_total[0]

    real_total, imaginary_total = lax.map(one_point, (masked_values, green_re, green_im, jnp.moveaxis(vertex_real, 2, 0), jnp.moveaxis(vert_im, 2, 0)))
    herm_re, herm_im = high_part(new_re, new_im)
    quad_re, quad_im = limit_term(masked_values, herm_re, herm_im)
    weight = tail_weight(NW)
    dens_re = (real_total + jnp.swapaxes(real_total, 1, 2)) / inverse_temp - weight * quad_re
    dens_im = (imaginary_total - jnp.swapaxes(imaginary_total, 1, 2)) / inverse_temp - weight * quad_im
    density = jnp.stack([dens_re, dens_im], axis=1)
    sigma_new = jnp.stack([new_re, new_im])
    return density, sigma_new
```

```python
import math

import jax
import jax.numpy as jnp
from jax import lax
from jax.experimental import pallas as pl
from jax.experimental.pallas import tpu as pltpu
from jax.sharding import Mesh
from jax.sharding import PartitionSpec as P

highest = lax.Precision.HIGHEST
inverse_temp = 40.0
LANES = 128
NN = (((1,), (0,)), ((), ()))
NT = (((1,), (1,)), ((), ()))


def tail_weight(count):
    total = 0.0
    for number in range(count):
        total += (inverse_temp / (math.pi * (2 * number + 1))) ** 2
    return inverse_temp / 4.0 - 2.0 / inverse_temp * total


def dot(a, b, dims, precision=highest):
    return lax.dot_general(a, b, dims, precision=precision, preferred_element_type=jnp.float32)


def split(x):
    high = x.astype(jnp.bfloat16)
    return high, (x - high.astype(jnp.float32)).astype(jnp.bfloat16)


def dot3(a, b, dims):
    return sum(
        lax.dot_general(x, y, dims, preferred_element_type=jnp.float32)
        for x, y in ((a[0], b[0]), (a[0], b[1]), (a[1], b[0]))
    )


def iota(shape, dim):
    return lax.broadcasted_iota(jnp.int32, shape, dim)


def matsubara(number):
    return (2.0 * number.astype(jnp.float32) + 1.0) * (math.pi / inverse_temp)


def masked_projector(proj_ref, window_ref):
    proj_re = proj_ref[0, 0]
    proj_im = proj_ref[0, 1]
    band = iota(proj_re.shape, 1)
    inside = (band >= window_ref[0, 0]) & (band < window_ref[0, 1])
    return jnp.where(inside, proj_re, 0.0), jnp.where(inside, proj_im, 0.0)


def invert(mat_re, mat_im):
    size = len(mat_re)
    mat_re, mat_im = list(mat_re), list(mat_im)
    column = iota(mat_re[0].shape, 0)
    for p in range(size):
        at = column == p
        piv_re = mat_re[p][p : p + 1]
        piv_im = mat_im[p][p : p + 1]
        rec = 1.0 / (piv_re * piv_re + piv_im * piv_im)
        rec_re = piv_re * rec
        rec_im = -piv_im * rec
        old_re = jnp.where(at, 1.0, mat_re[p])
        old_im = jnp.where(at, 0.0, mat_im[p])
        row_re = old_re * rec_re - old_im * rec_im
        row_im = old_re * rec_im + old_im * rec_re
        for i in range(size):
            if i == p:
                continue
            col_re = mat_re[i][p : p + 1]
            col_im = mat_im[i][p : p + 1]
            rest_re = jnp.where(at, 0.0, mat_re[i])
            rest_im = jnp.where(at, 0.0, mat_im[i])
            mat_re[i] = rest_re - (col_re * row_re - col_im * row_im)
            mat_im[i] = rest_im - (col_re * row_im + col_im * row_re)
        mat_re[p] = row_re
        mat_im[p] = row_im
    return mat_re, mat_im


def cmul(first_re, first_im, second_re, second_im):
    size = len(first_re)
    out_re, out_im = [], []
    for i in range(size):
        sum_re = sum_im = 0.0
        for k in range(size):
            a_re = first_re[i][k : k + 1]
            a_im = first_im[i][k : k + 1]
            sum_re = sum_re + (a_re * second_re[k] - a_im * second_im[k])
            sum_im = sum_im + (a_re * second_im[k] + a_im * second_re[k])
        out_re.append(sum_re)
        out_im.append(sum_im)
    return out_re, out_im


def rows_of(block, norb):
    return [block[norb * i : norb * (i + 1)] for i in range(norb)]


def turned(ref, first, chips, freqs, pitch):
    rows = [ref[pl.ds(first + f, chips, stride=pitch), :] for f in range(freqs)]
    return jnp.concatenate(rows, axis=0).T


def project_kernel(norb, chips, freqs, core_axis, energy_ref, proj_ref, window_ref, out_ref):
    core = lax.axis_index(core_axis)
    proj_re, proj_im = masked_projector(proj_ref, window_ref)
    pair = iota((LANES, norb), 0)
    orb = iota((LANES, norb), 1)
    first = sum((pair >= norb * t).astype(jnp.int32) for t in range(1, norb))
    inside = pair < norb * norb
    pick_i = jnp.where((first == orb) & inside, 1.0, 0.0)
    pick_j = jnp.where((pair - norb * first == orb) & inside, 1.0, 0.0)
    i_re, i_im = dot(pick_i, proj_re, NN), dot(pick_i, proj_im, NN)
    j_re, j_im = dot(pick_j, proj_re, NN), dot(pick_j, proj_im, NN)
    pair_re = i_re * j_re + i_im * j_im
    pair_im = i_im * j_re - i_re * j_im
    energy = energy_ref[...]
    group = 2 * freqs
    rows = chips * group
    for other in range(2):
        row = iota((rows, energy.shape[1]), 0)
        chip = row // group
        place = row - group * chip
        half = place // freqs
        number = 2 * freqs * chip + freqs * (core ^ other) + place - freqs * half
        freq = matsubara(number)
        denom = energy * energy + freq * freq
        green_re = -energy / denom
        green_im = -freq / denom
        real = half == 0
        total = dot(jnp.where(real, green_re, green_im), pair_re, NT) + dot(
            jnp.where(real, -green_im, green_re), pair_im, NT
        )
        out_ref[:, group * other : group * (other + 1), :] = total.reshape(chips, group, LANES)


def dyson_kernel(
    norb, chips, freqs, points, own_ref, sib_ref, sigma_ref, imp_ref, new_ref, tile_ref,
    mat_ref, sum_ref, small_ref, wide_ref, turn_ref,
):
    pairs = norb * norb
    group = 2 * freqs
    for half in range(2):
        mat_ref[half, :, :LANES] = turned(own_ref, freqs * half, chips, freqs, 2 * group)
        mat_ref[half, :, LANES:] = turned(sib_ref, freqs * half, chips, freqs, group)
    for which, ref in enumerate((sigma_ref, imp_ref)):
        for half in range(2):
            for i in range(norb):
                at = (which * 2 + half) * pairs + norb * i
                small_ref[at : at + norb, :] = ref[half, i]
    spread = jnp.where(iota((freqs, LANES), 1) // chips == iota((freqs, LANES), 0), 1.0, 0.0)
    wide_ref[...] = dot(small_ref[...], spread, NN)

    def rows(ref, base):
        return [ref[base + norb * i : base + norb * (i + 1), :] for i in range(norb)]

    sig_re, sig_im = rows(wide_ref, 0), rows(wide_ref, pairs)
    for part in range(2):
        lanes = pl.ds(LANES * part, LANES)
        mat = [
            [mat_ref[half, norb * i : norb * (i + 1), lanes] for i in range(norb)]
            for half in range(2)
        ]
        ainv_re, ainv_im = invert(*mat)
        gorb_re, gorb_im = invert(
            [a - s for a, s in zip(ainv_re, sig_re)], [a - s for a, s in zip(ainv_im, sig_im)]
        )
        for i in range(norb):
            sum_ref[norb * i : norb * (i + 1), lanes] = gorb_re[i]
            sum_ref[pairs + norb * i : pairs + norb * (i + 1), lanes] = gorb_im[i]
    both = sum_ref[:, :LANES] + sum_ref[:, LANES:]
    same = iota((LANES, LANES), 0) // chips == iota((LANES, LANES), 1) // chips
    sum_ref[:, :LANES] = dot(both, jnp.where(same, 1.0 / points, 0.0), NN)
    loc = [
        [sum_ref[base + norb * i : base + norb * (i + 1), :LANES] for i in range(norb)]
        for base in (0, pairs)
    ]
    inv = invert(*loc)
    imp = rows(wide_ref, 2 * pairs), rows(wide_ref, 3 * pairs)
    pitch = turn_ref.shape[1] // norb
    diff = [[v - m for v, m in zip(inv[half], imp[half])] for half in range(2)]
    for half in range(2):
        for i in range(norb):
            turn_ref[half, pitch * i : pitch * i + norb, :] = diff[half][i]
    mat_ref[...] = jnp.zeros_like(mat_ref)
    for half, sig, sign in ((0, sig_re, 1.0), (1, sig_im, -1.0)):
        for i in range(norb):
            across = turn_ref[half, pl.ds(i, norb, stride=pitch), :]
            fresh = sig[i] + 0.5 * (diff[half][i] + sign * across)
            mat_ref[half, norb * i : norb * (i + 1), :LANES] = fresh
    lane = iota((LANES, freqs), 0)
    pick = jnp.where(lane == chips * iota((LANES, freqs), 1), 1.0, 0.0)
    for half in range(2):
        few = dot(mat_ref[half, :, :LANES], pick, NN)
        for i in range(norb):
            new_ref[half, i] = few[norb * i : norb * (i + 1)]
    row = iota((group, LANES), 0)
    lane = iota((group, LANES), 1)
    tile = 0.0
    for half in range(2):
        choose = jnp.where(lane == chips * (row - freqs * half), 1.0, 0.0)
        tile = tile + dot(choose, mat_ref[half, :, :LANES], NT)
    tile_ref[...] = jnp.broadcast_to(tile[None], tile_ref.shape)


def density_kernel(
    norb, chips, freqs, core_axis, energy_ref, proj_ref, window_ref, mat_ref, own_ref, sib_ref,
    out_ref, flat_ref, ainv_ref, sig_ref, vert_ref, sums_ref,
):
    core = lax.axis_index(core_axis)
    group = 2 * freqs
    bands = energy_ref.shape[1]
    count = 2 * freqs * chips
    tall = -(-bands // 16) * 16
    pad = flat_ref.shape[1] // 8
    proj_re, proj_im = masked_projector(proj_ref, window_ref)
    flat_ref[...] = jnp.zeros_like(flat_ref)
    step = 16
    flat_ref[0:norb, :bands] = proj_re
    flat_ref[step : step + norb, :bands] = proj_im
    flat_ref[2 * step : 2 * step + 1, :bands] = energy_ref[...]
    upright = flat_ref[...].T[:tall]
    flat_ref[...] = jnp.zeros_like(flat_ref)
    flat_ref[0:norb, :bands] = -proj_im
    flat_ref[step : step + norb, :bands] = proj_re
    crossed = flat_ref[...].T[:tall]
    energy = upright[:, 2 * step : 2 * step + 1]
    lane = iota((tall, count), 1)
    part = lane // LANES
    within = lane - LANES * part
    place = within // chips
    number = 2 * freqs * (within - chips * place) + freqs * (core ^ part) + place
    freq = matsubara(number)
    denom = energy * energy + freq * freq
    green_re = -energy / denom
    green_im = -freq / denom
    last = number[:norb] == count - 1

    for part in range(2):
        lanes = pl.ds(LANES * part, LANES)
        for half in range(2):
            ainv_ref[half] = turned(mat_ref, group * part + freqs * half, chips, freqs, 2 * group)
            sig_ref[half, :, lanes] = turned(
                (own_ref, sib_ref)[part], freqs * half, chips, freqs, group
            )
        mat = [
            [ainv_ref[half, norb * i : norb * (i + 1), :] for i in range(norb)] for half in range(2)
        ]
        sig = [
            [sig_ref[half, norb * i : norb * (i + 1), lanes] for i in range(norb)]
            for half in range(2)
        ]
        inv = invert(*mat)
        dressed = invert(
            [a - s for a, s in zip(inv[0], sig[0])], [a - s for a, s in zip(inv[1], sig[1])]
        )
        whole = cmul(*cmul(*sig, *dressed), *sig)
        for i in range(norb):
            spot = pl.ds(count * i + LANES * part, LANES)
            vert_ref[0:norb, spot] = sig[0][i] + whole[0][i]
            vert_ref[step : step + norb, spot] = sig[1][i] + whole[1][i]

    spare = jnp.zeros((step - norb, norb * count), jnp.float32)
    vert_ref[norb:step] = spare
    vert_ref[step + norb : 2 * step] = spare
    orb = iota((norb, LANES), 1)
    ends = []
    for half in range(2):
        end = jnp.zeros((norb, LANES), jnp.float32)
        for i in range(norb):
            entry = jnp.where(last, sig_ref[half, norb * i : norb * (i + 1), :], 0.0)
            end = jnp.where(orb == i, jnp.sum(entry, axis=1, keepdims=True), end)
        ends.append(end)
        ends.append(jnp.zeros((step - norb, LANES), jnp.float32))
    end = jnp.concatenate(ends, axis=0)

    wide = 2 * step
    plus = upright[:, :wide]
    cross = crossed[:, :wide]
    to_re = jnp.where(iota(plus.shape, 1) < step, plus, -plus)
    to_im = jnp.where(iota(plus.shape, 1) < step, -cross, cross)
    left = jnp.concatenate([to_re, to_im], axis=0)
    left_parts = split(left)
    left_all = jnp.concatenate([left_parts[0], left_parts[0], left_parts[1]], axis=1)

    weight = -0.5 * inverse_temp * tail_weight(count)
    tail = weight * dot(left, end, NN)
    tail_re, tail_im = tail[:tall], tail[tall:]
    slot = iota((tall, LANES), 1) < norb
    side_re = jnp.where(slot, upright, 0.0)
    side_im = jnp.where(slot, crossed, 0.0)
    side_re, side_im, tail_re, tail_im = (split(x) for x in (side_re, side_im, tail_re, tail_im))

    total_re = dot3(side_re, tail_re, NT) - dot3(side_im, tail_im, NT)
    total_im = dot3(side_re, tail_im, NT) + dot3(side_im, tail_re, NT)
    for i in range(norb):
        vert = split(vert_ref[:, count * i : count * (i + 1)])
        vert_all = jnp.concatenate([vert[0], vert[1], vert[0]], axis=0)
        mixed = lax.dot_general(left_all, vert_all, NN, preferred_element_type=jnp.float32)
        mix_re, mix_im = mixed[:tall], mixed[tall:]
        right_re = mix_re * green_re - mix_im * green_im
        right_im = mix_re * green_im + mix_im * green_re
        p_re = upright[:, i : i + 1]
        p_im = -crossed[:, i : i + 1]
        side_re = green_re * p_re + green_im * p_im
        side_im = green_im * p_re - green_re * p_im
        side = split(jnp.concatenate([side_re, side_im], axis=1))
        total_re = total_re + dot3(side, split(jnp.concatenate([right_re, -right_im], axis=1)), NT)
        total_im = total_im + dot3(side, split(jnp.concatenate([right_im, right_re], axis=1)), NT)
    sums_ref[...] = jnp.zeros_like(sums_ref)
    for half, total, sign in ((0, total_re, 1.0), (1, total_im, -1.0)):
        sums_ref[:tall, :tall] = total
        both = sums_ref[...] + sign * sums_ref[...].T
        out_ref[0, half] = both[:bands, :bands] / inverse_temp


VMEM = pl.BlockSpec(memory_space=pltpu.VMEM)
SMEM = pl.BlockSpec(memory_space=pltpu.SMEM)


def f32(*shape):
    return jax.ShapeDtypeStruct(shape, jnp.float32)


def scratch(*shape):
    return pltpu.VMEM(shape, jnp.float32)


def local(energies, proj, window, sigma, impurity_inverse):
    norb = proj.shape[2]
    bands = energies.shape[1]
    freqs = sigma.shape[3]
    chips = lax.axis_size("z")
    cores = lax.axis_size("core")
    group = 2 * freqs
    pairs = norb * norb
    count = freqs * chips * cores
    points = energies.shape[0] * chips * cores
    swap = [(0, 1), (1, 0)]
    wide = -(-bands // LANES) * LANES
    roomy = pltpu.CompilerParams(vmem_limit_bytes=48 * 1024 * 1024)

    def run(body, out, specs, scratches=()):
        return pl.pallas_call(
            body,
            out_shape=out,
            in_specs=specs,
            out_specs=jax.tree.map(lambda _: VMEM, out),
            scratch_shapes=scratches,
            compiler_params=roomy,
        )

    def project(*refs):
        project_kernel(norb, chips, freqs, "core", *refs)

    def dyson(*refs):
        dyson_kernel(norb, chips, freqs, points, *refs)

    def rebuild(*refs):
        density_kernel(norb, chips, freqs, "core", *refs)

    mats = run(project, f32(chips, 2 * group, LANES), [VMEM, VMEM, SMEM])(energies, proj, window)
    got = lax.all_to_all(mats, "z", 0, 0, tiled=True)
    sib = lax.ppermute(got[:, group:], "core", swap)
    sigma_new, tiles = run(
        dyson,
        (f32(2, norb, norb, freqs), f32(chips, group, LANES)),
        [VMEM] * 4,
        [
            scratch(2, LANES, 2 * LANES),
            scratch(2 * pairs, 2 * LANES),
            scratch(4 * pairs, freqs),
            scratch(4 * pairs, LANES),
            scratch(2, 16 * norb, LANES),
        ],
    )(got.reshape(-1, LANES), sib.reshape(-1, LANES), sigma, impurity_inverse)
    own = lax.all_to_all(tiles, "z", 0, 0, tiled=True)
    sib = lax.ppermute(own, "core", swap)
    density = run(
        rebuild,
        f32(1, 2, bands, bands),
        [VMEM, VMEM, SMEM, VMEM, VMEM, VMEM],
        [
            scratch(LANES, wide),
            scratch(2, LANES, LANES),
            scratch(2, LANES, 2 * LANES),
            scratch(32, norb * count),
            scratch(wide, wide),
        ],
    )(
        energies,
        proj,
        window,
        mats.reshape(-1, LANES),
        own.reshape(-1, LANES),
        sib.reshape(-1, LANES),
    )
    return density, sigma_new


def solution(mesh):
    parts, line = mesh.shape["parts"], mesh.shape["ka"]
    torus = Mesh(mesh.devices.reshape(parts, line // 2, 2), ("parts", "z", "core"))
    every = ("parts", "z", "core")
    line = ("z", "core")
    in_specs = (
        P(every, None),
        P(every, None, None, None),
        P(every, None),
        P("parts", None, None, line),
        P("parts", None, None, line),
    )
    out_specs = (P(every, None, None, None), P("parts", None, None, line))
    return jax.shard_map(local, mesh=torus, in_specs=in_specs, out_specs=out_specs, check_vma=False)
```

```python
import math

import jax
import jax.numpy as jnp
from jax import lax
from jax.experimental import pallas as pl
from jax.experimental.pallas import tpu as pltpu
from jax.sharding import Mesh
from jax.sharding import PartitionSpec as P

highest = lax.Precision.HIGHEST
inverse_temp = 40.0
LANES = 128
NN = (((1,), (0,)), ((), ()))
NT = (((1,), (1,)), ((), ()))


def tail_weight(count):
    total = 0.0
    for number in range(count):
        total += (inverse_temp / (math.pi * (2 * number + 1))) ** 2
    return inverse_temp / 4.0 - 2.0 / inverse_temp * total


def dot(a, b, dims, precision=highest):
    return lax.dot_general(a, b, dims, precision=precision, preferred_element_type=jnp.float32)


def split(x):
    high = x.astype(jnp.bfloat16)
    return high, (x - high.astype(jnp.float32)).astype(jnp.bfloat16)


def dot3(a, b, dims):
    return sum(
        lax.dot_general(x, y, dims, preferred_element_type=jnp.float32)
        for x, y in ((a[0], b[0]), (a[0], b[1]), (a[1], b[0]))
    )


def iota(shape, dim):
    return lax.broadcasted_iota(jnp.int32, shape, dim)


def matsubara(number):
    return (2.0 * number.astype(jnp.float32) + 1.0) * (math.pi / inverse_temp)


def spare_of(norb):
    used = norb * norb
    width = LANES - used
    pieces = -(-used // width)
    return used, width, pieces


def kept_rows(norb, rows):
    pieces = spare_of(norb)[2]
    extra = 0
    while pieces * (extra + 1) <= rows - (extra + 1):
        extra += 1
    return rows - extra


def pack(rows, norb):
    used, width, pieces = spare_of(norb)
    kept = kept_rows(norb, len(rows))
    out = list(rows[:kept])
    lane = iota(rows[0].shape, 1)
    for e, row in enumerate(rows[kept:]):
        for p in range(pieces):
            moved = pltpu.roll(row, (used - width * p) % LANES, 1)
            out[pieces * e + p] = jnp.where(lane < used, out[pieces * e + p], moved)
    return out


def unpack(kept, norb, rows):
    used, width, pieces = spare_of(norb)
    out = list(kept)
    lane = iota(kept[0].shape, 1)
    for e in range(rows - len(kept)):
        row = 0.0
        for p in range(pieces):
            moved = pltpu.roll(kept[pieces * e + p], (width * p - used) % LANES, 1)
            inside = (lane >= width * p) & (lane < min(width * (p + 1), used))
            row = jnp.where(inside, moved, row)
        out.append(row)
    return out


def spaced(ref, chips, norb, rows):
    pitch = kept_rows(norb, rows)
    return unpack([ref[pl.ds(r, chips, stride=pitch), :] for r in range(pitch)], norb, rows)


def upright(rows):
    return jnp.concatenate(rows, axis=0).T


def band_inside(shape, window_ref):
    band = iota(shape, 1)
    return (band >= window_ref[0, 0]) & (band < window_ref[0, 1])


def invert(mat_re, mat_im):
    size = len(mat_re)
    mat_re, mat_im = list(mat_re), list(mat_im)
    column = iota(mat_re[0].shape, 0)
    for p in range(size):
        at = column == p
        piv_re = mat_re[p][p : p + 1]
        piv_im = mat_im[p][p : p + 1]
        rec = 1.0 / (piv_re * piv_re + piv_im * piv_im)
        rec_re = piv_re * rec
        rec_im = -piv_im * rec
        old_re = jnp.where(at, 1.0, mat_re[p])
        old_im = jnp.where(at, 0.0, mat_im[p])
        row_re = old_re * rec_re - old_im * rec_im
        row_im = old_re * rec_im + old_im * rec_re
        for i in range(size):
            if i == p:
                continue
            col_re = mat_re[i][p : p + 1]
            col_im = mat_im[i][p : p + 1]
            rest_re = jnp.where(at, 0.0, mat_re[i])
            rest_im = jnp.where(at, 0.0, mat_im[i])
            mat_re[i] = rest_re - (col_re * row_re - col_im * row_im)
            mat_im[i] = rest_im - (col_re * row_im + col_im * row_re)
        mat_re[p] = row_re
        mat_im[p] = row_im
    return mat_re, mat_im


def rows_of(block, norb):
    return [block[norb * i : norb * (i + 1)] for i in range(norb)]


def project_kernel(
    norb, chips, freqs, core_axis, energy_ref, proj_ref, window_ref, packed_ref, plain_ref, flat_ref
):
    core = lax.axis_index(core_axis)
    for i in range(norb):
        flat_ref[2 * i : 2 * i + 2, :] = proj_ref[0, i]
    flat = jnp.where(band_inside(flat_ref.shape, window_ref), flat_ref[...], 0.0)
    pair = iota((LANES, 2 * norb), 0)
    orb = iota((LANES, 2 * norb), 1)
    first = sum((pair >= norb * t).astype(jnp.int32) for t in range(1, norb))
    second = pair - norb * first
    inside = pair < norb * norb
    picks = [
        jnp.where((2 * which + half == orb) & inside, 1.0, 0.0)
        for which in (first, second)
        for half in range(2)
    ]
    picked = dot(jnp.concatenate(picks, axis=0), flat, NN)
    i_re, i_im, j_re, j_im = (picked[LANES * k : LANES * (k + 1)] for k in range(4))
    pair_re = i_re * j_re + i_im * j_im
    pair_im = i_im * j_re - i_re * j_im
    energy = energy_ref[...]
    rows = freqs * chips
    row = iota((rows, energy.shape[1]), 0)
    place = row // chips
    lines = []
    for other in range(2):
        number = 2 * freqs * (row - chips * place) + freqs * (core ^ other) + place
        freq = matsubara(number)
        denom = 1.0 / (energy * energy + freq * freq)
        green_re = -energy * denom
        green_im = -freq * denom
        for left, right in ((green_re, -green_im), (green_im, green_re)):
            total = dot(left, pair_re, NT) + dot(right, pair_im, NT)
            at = rows * (len(lines) // freqs)
            plain_ref[at : at + rows, :] = total
            lines += [total[chips * f : chips * (f + 1)] for f in range(freqs)]
    lines = pack(lines, norb)
    for r, line in enumerate(lines):
        packed_ref[pl.ds(r, chips, stride=len(lines)), :] = line


def dyson_kernel(
    norb, chips, freqs, points, own_ref, sib_ref, sigma_ref, imp_ref, new_ref, tile_ref,
    mat_ref, sum_ref, small_ref, wide_ref, turn_ref,
):
    pairs = norb * norb
    group = 2 * freqs
    lines = spaced(own_ref, chips, norb, 2 * group)[:group]
    lines += spaced(sib_ref, chips, norb, 2 * group)[group:]
    for half in range(2):
        for part in range(2):
            at = group * part + freqs * half
            mat_ref[half, :, LANES * part : LANES * (part + 1)] = upright(lines[at : at + freqs])
    for which, ref in enumerate((sigma_ref, imp_ref)):
        for half in range(2):
            for i in range(norb):
                at = (which * 2 + half) * pairs + norb * i
                small_ref[at : at + norb, :] = ref[half, i]
    spread = jnp.where(iota((freqs, LANES), 1) // chips == iota((freqs, LANES), 0), 1.0, 0.0)
    wide_ref[...] = dot(small_ref[...], spread, NN)

    def rows(ref, base):
        return [ref[base + norb * i : base + norb * (i + 1), :] for i in range(norb)]

    sig_re, sig_im = rows(wide_ref, 0), rows(wide_ref, pairs)
    for part in range(2):
        lanes = pl.ds(LANES * part, LANES)
        mat = [
            [mat_ref[half, norb * i : norb * (i + 1), lanes] for i in range(norb)]
            for half in range(2)
        ]
        ainv_re, ainv_im = invert(*mat)
        gorb_re, gorb_im = invert(
            [a - s for a, s in zip(ainv_re, sig_re)], [a - s for a, s in zip(ainv_im, sig_im)]
        )
        for i in range(norb):
            sum_ref[norb * i : norb * (i + 1), lanes] = gorb_re[i]
            sum_ref[pairs + norb * i : pairs + norb * (i + 1), lanes] = gorb_im[i]
    both = sum_ref[:, :LANES] + sum_ref[:, LANES:]
    same = iota((LANES, LANES), 0) // chips == iota((LANES, LANES), 1) // chips
    sum_ref[:, :LANES] = dot(both, jnp.where(same, 1.0 / points, 0.0), NN)
    loc = [
        [sum_ref[base + norb * i : base + norb * (i + 1), :LANES] for i in range(norb)]
        for base in (0, pairs)
    ]
    inv = invert(*loc)
    imp = rows(wide_ref, 2 * pairs), rows(wide_ref, 3 * pairs)
    pitch = turn_ref.shape[1] // norb
    diff = [[v - m for v, m in zip(inv[half], imp[half])] for half in range(2)]
    for half in range(2):
        for i in range(norb):
            turn_ref[half, pitch * i : pitch * i + norb, :] = diff[half][i]
    mat_ref[...] = jnp.zeros_like(mat_ref)
    for half, sig, sign in ((0, sig_re, 1.0), (1, sig_im, -1.0)):
        for i in range(norb):
            across = turn_ref[half, pl.ds(i, norb, stride=pitch), :]
            fresh = sig[i] + 0.5 * (diff[half][i] + sign * across)
            mat_ref[half, norb * i : norb * (i + 1), :LANES] = fresh
    row = iota((group, LANES), 0)
    lane = iota((group, LANES), 1)
    tile = 0.0
    for half in range(2):
        choose = jnp.where(lane == chips * (row - freqs * half), 1.0, 0.0)
        tile = tile + dot(choose, mat_ref[half, :, :LANES], NT)
    for half in range(2):
        for i in range(norb):
            new_ref[half, i] = tile[freqs * half : freqs * (half + 1), norb * i : norb * (i + 1)]
    lines = pack([tile[r : r + 1] for r in range(group)], norb)
    for r, line in enumerate(lines):
        tile_ref[pl.ds(r, chips, stride=len(lines)), :] = jnp.broadcast_to(line, (chips, LANES))


def numbers(shape, chips, freqs, core):
    lane = iota(shape, 1)
    part = lane // LANES
    within = lane - LANES * part
    place = within // chips
    return 2 * freqs * (within - chips * place) + freqs * (core ^ part) + place


STEP = 16


def prepare_kernel(
    norb, chips, freqs, core_axis, energy_ref, proj_ref, window_ref, plain_ref,
    ainv_ref, green_ref, left_ref, side_ref, right_ref, flat_ref,
):
    core = lax.axis_index(core_axis)
    bands = energy_ref.shape[1]
    tall = green_ref.shape[1]
    count = green_ref.shape[2]
    rows = freqs * chips
    for part in range(2):
        mat = []
        for half in range(2):
            at = rows * (2 * part + half)
            turned = plain_ref[at : at + rows, :].T
            mat.append(rows_of(turned, norb))
        inv = invert(*mat)
        for half in range(2):
            for i in range(norb):
                ainv_ref[2 * half + part, norb * i : norb * (i + 1), :] = inv[half][i]

    flat_ref[...] = jnp.zeros_like(flat_ref)
    for i in range(norb):
        flat_ref[i : i + 1, :bands] = proj_ref[0, i, 0:1]
        flat_ref[STEP + i : STEP + i + 1, :bands] = proj_ref[0, i, 1:2]
    flat_ref[2 * STEP : 2 * STEP + 1, :bands] = energy_ref[...]
    keep = band_inside(flat_ref.shape, window_ref) | (iota(flat_ref.shape, 0) >= 2 * STEP)
    turned = jnp.where(keep, flat_ref[...], 0.0).T[:tall]
    energy = turned[:, 2 * STEP : 2 * STEP + 1]
    freq = matsubara(numbers((tall, count), chips, freqs, core))
    denom = 1.0 / (energy * energy + freq * freq)
    green_re = -energy * denom
    green_im = -freq * denom
    green_ref[0] = green_re
    green_ref[1] = green_im
    wide = 2 * STEP
    straight = turned[:, :wide]
    crossed = jnp.concatenate([turned[:, STEP:wide], turned[:, :STEP]], axis=1)
    early = iota(straight.shape, 1) < STEP
    left = jnp.concatenate([straight, jnp.where(early, -crossed, crossed)], axis=0)
    high, low = split(left)
    left_ref[...] = jnp.concatenate([high, high, low], axis=1)
    side_ref[:, :wide] = straight
    side_ref[:, wide:] = crossed
    for j in range(norb):
        p_re = turned[:, j : j + 1]
        p_im = turned[:, STEP + j : STEP + j + 1]
        re = split(green_re * p_re - green_im * p_im)
        im = split(green_re * p_im + green_im * p_re)
        for k in range(2):
            right_ref[j, :, 2 * count * k : 2 * count * k + count] = re[k]
            right_ref[j, :, 2 * count * k + count : 2 * count * (k + 1)] = im[k]


def solve(mat, rhs):
    size = len(mat[0])
    mat = [list(m) for m in mat]
    out = [list(r) for r in rhs]
    row = iota(mat[0][0].shape, 0)
    for p in range(size):
        at = row == p
        piv_re = mat[0][p][p : p + 1]
        piv_im = mat[1][p][p : p + 1]
        rec = 1.0 / (piv_re * piv_re + piv_im * piv_im)
        rec_re = piv_re * rec
        rec_im = -piv_im * rec
        old_re = jnp.where(at, -1.0, mat[0][p])
        old_im = jnp.where(at, 0.0, mat[1][p])
        col_re = old_re * rec_re - old_im * rec_im
        col_im = old_re * rec_im + old_im * rec_re
        for cols, start in ((mat, p + 1), (out, 0)):
            for q in range(start, size):
                x_re = cols[0][q][p : p + 1]
                x_im = cols[1][q][p : p + 1]
                rest_re = jnp.where(at, 0.0, cols[0][q])
                rest_im = jnp.where(at, 0.0, cols[1][q])
                cols[0][q] = rest_re - (col_re * x_re - col_im * x_im)
                cols[1][q] = rest_im - (col_re * x_im + col_im * x_re)
    return out


def density_kernel(
    norb, chips, freqs, core_axis, ainv_ref, green_ref, left_ref, side_ref, right_ref, own_ref, sib_ref,
    out_ref, sig_ref, vert_ref, sums_ref, held_ref, done,
):
    core = lax.axis_index(core_axis)
    fetch = pltpu.make_async_copy(right_ref, held_ref, done)
    fetch.start()
    group = 2 * freqs
    bands = out_ref.shape[2]
    tall = green_ref.shape[1]
    count = green_ref.shape[2]
    wide = 2 * STEP
    for part in range(2):
        lines = spaced((own_ref, sib_ref)[part], chips, norb, group)
        for half in range(2):
            sig_ref[2 * half + part] = upright(lines[freqs * half : freqs * (half + 1)])

    def columns(ref, half, part):
        return [ref[2 * half + part, pl.ds(j, norb, stride=norb), :] for j in range(norb)]

    spare = jnp.zeros((STEP - norb, norb * count), jnp.float32)
    vert_ref[norb:STEP] = spare
    vert_ref[STEP + norb : wide] = spare
    for part in range(2):
        sig = [columns(sig_ref, half, part) for half in range(2)]
        mat = [
            [a - s for a, s in zip(columns(ainv_ref, half, part), sig[half])] for half in range(2)
        ]
        turned = solve(mat, sig)
        for j in range(norb):
            sum_re, sum_im = sig[0][j], sig[1][j]
            for k in range(norb):
                y_re = turned[0][j][k : k + 1]
                y_im = turned[1][j][k : k + 1]
                sum_re = sum_re + (sig[0][k] * y_re - sig[1][k] * y_im)
                sum_im = sum_im + (sig[0][k] * y_im + sig[1][k] * y_re)
            spot = pl.ds(count * j + LANES * part, LANES)
            vert_ref[0:norb, spot] = sum_re
            vert_ref[STEP : STEP + norb, spot] = sum_im

    last = numbers((norb, count), chips, freqs, core) == count - 1
    orb = iota((norb, LANES), 1)
    ends = []
    for half in range(2):
        end = jnp.zeros((norb, LANES), jnp.float32)
        for j in range(norb):
            for part in range(2):
                spot = last[:, LANES * part : LANES * (part + 1)]
                entry = jnp.where(spot, columns(sig_ref, half, part)[j], 0.0)
                end = end + jnp.where(orb == j, jnp.sum(entry, axis=1, keepdims=True), 0.0)
        ends += [end, jnp.zeros((STEP - norb, LANES), jnp.float32)]
    left = left_ref[...]

    def mixed(block):
        high, low = split(block)
        stacked = jnp.concatenate([high, low, high], axis=0)
        return lax.dot_general(left, stacked, NN, preferred_element_type=jnp.float32)

    def join(re, im, right):
        re, im = split(re), split(im)
        top = [jnp.concatenate([re[k], -im[k]], axis=1) for k in range(2)]
        low = [jnp.concatenate([im[k], re[k]], axis=1) for k in range(2)]
        line = [jnp.concatenate([t, b], axis=0) for t, b in zip(top, low)]
        return dot3(line, right, NT)

    weight = -0.5 * inverse_temp * tail_weight(count)
    tail = weight * mixed(jnp.concatenate(ends, axis=0))
    side = side_ref[...]
    orbs = jnp.zeros((tall, LANES - STEP), jnp.float32)
    right = split(jnp.concatenate([side[:, :STEP], orbs, side[:, wide : wide + STEP], orbs], axis=1))
    total = join(tail[:tall], tail[tall:], right)
    fetch.wait()
    for j in range(norb):
        mix = mixed(vert_ref[:, count * j : count * (j + 1)])
        mix_re, mix_im = mix[:tall], mix[tall:]
        side_re = mix_re * green_ref[0] - mix_im * green_ref[1]
        side_im = mix_re * green_ref[1] + mix_im * green_ref[0]
        right = [held_ref[j, :, 2 * count * k : 2 * count * (k + 1)] for k in range(2)]
        total = total + join(side_re, side_im, right)
    sums_ref[...] = jnp.zeros_like(sums_ref)
    for half, sign in ((0, 1.0), (1, -1.0)):
        sums_ref[:tall, :tall] = total[tall * half : tall * (half + 1)]
        both = sums_ref[...] + sign * sums_ref[...].T
        out_ref[0, half] = both[:bands, :bands] / inverse_temp


BLOCK = pl.BlockSpec()
VMEM = pl.BlockSpec(memory_space=pltpu.VMEM)
SMEM = pl.BlockSpec(memory_space=pltpu.SMEM)


def struct(*shape, dtype=jnp.float32):
    return jax.ShapeDtypeStruct(shape, dtype)


def scratch(*shape):
    return pltpu.VMEM(shape, jnp.float32)


def run(body, out, specs, scratches=()):
    return pl.pallas_call(
        body,
        out_shape=out,
        in_specs=specs,
        out_specs=jax.tree.map(lambda _: VMEM, out),
        scratch_shapes=scratches,
        compiler_params=pltpu.CompilerParams(vmem_limit_bytes=32 * 1024 * 1024),
    )


def kernels(norb, bands, freqs, chips, cores, points):
    group = 2 * freqs
    pairs = norb * norb
    count = freqs * chips * cores
    wide = -(-bands // LANES) * LANES
    tall = -(-bands // 16) * 16
    long = kept_rows(norb, 2 * group)
    short = kept_rows(norb, group)
    axis = "core"

    def project(*refs):
        project_kernel(norb, chips, freqs, axis, *refs)

    def dyson(*refs):
        dyson_kernel(norb, chips, freqs, points, *refs)

    def prepare(*refs):
        prepare_kernel(norb, chips, freqs, axis, *refs)

    def rebuild(*refs):
        density_kernel(norb, chips, freqs, axis, *refs)

    first = run(
        project,
        (struct(chips * long, LANES), struct(2 * count, LANES)),
        [BLOCK, BLOCK, SMEM],
        [scratch(2 * norb, bands)],
    )
    second = run(
        dyson,
        (struct(2, norb, freqs, norb), struct(chips * short, LANES)),
        [VMEM] * 4,
        [
            scratch(2, LANES, 2 * LANES),
            scratch(2 * pairs, 2 * LANES),
            scratch(4 * pairs, freqs),
            scratch(4 * pairs, LANES),
            scratch(2, 16 * norb, LANES),
        ],
    )
    aside = run(
        prepare,
        (
            struct(4, pairs, LANES),
            struct(2, tall, count),
            struct(2 * tall, 6 * STEP, dtype=jnp.bfloat16),
            struct(tall, 4 * STEP),
            struct(norb, tall, 4 * count, dtype=jnp.bfloat16),
        ),
        [BLOCK, BLOCK, SMEM, VMEM],
        [scratch(LANES, wide)],
    )
    third = run(
        rebuild,
        struct(1, 2, bands, bands),
        [VMEM] * 4 + [pl.BlockSpec(memory_space=pl.ANY)] + [VMEM] * 2,
        [
            scratch(4, LANES, LANES),
            scratch(2 * STEP, norb * count),
            scratch(wide, wide),
            pltpu.VMEM((norb, tall, 4 * count), jnp.bfloat16),
            pltpu.SemaphoreType.DMA(()),
        ],
    )
    return first, aside, second, third


def local(energies, proj, window, sigma, impurity_inverse):
    norb, bands = proj.shape[2:]
    freqs = sigma.shape[3]
    chips = lax.axis_size("z")
    cores = lax.axis_size("core")
    points = energies.shape[0] * chips * cores
    first, aside, second, third = kernels(norb, bands, freqs, chips, cores, points)
    swap = [(0, 1), (1, 0)]
    proj = jnp.swapaxes(proj, 1, 2)

    def across(rows):
        got = lax.all_to_all(rows.reshape(chips, 1, -1), "z", 0, 0, tiled=True)
        return got.reshape(rows.shape)

    packed, plain = first(energies, proj, window)
    ready = aside(energies, proj, window, plain)
    got, ready = lax.optimization_barrier((across(packed), ready))
    sigma_new, tiles = second(got, lax.ppermute(got, "core", swap), sigma, impurity_inverse)
    back = across(tiles)
    density = third(*ready, back, lax.ppermute(back, "core", swap))
    return density, jnp.swapaxes(sigma_new, 2, 3)


def solution(mesh):
    parts, line = mesh.shape["parts"], mesh.shape["ka"]
    torus = Mesh(mesh.devices.reshape(parts, line // 2, 2), ("parts", "z", "core"))
    every = ("parts", "z", "core")
    line = ("z", "core")
    in_specs = (
        P(every, None),
        P(every, None, None, None),
        P(every, None),
        P("parts", None, None, line),
        P("parts", None, None, line),
    )
    out_specs = (P(every, None, None, None), P("parts", None, None, line))
    return jax.shard_map(local, mesh=torus, in_specs=in_specs, out_specs=out_specs, check_vma=False)
```

```python
import math

import jax
import jax.numpy as jnp
from jax import lax
from jax.experimental import pallas as pl
from jax.experimental.pallas import tpu as pltpu
from jax.sharding import Mesh
from jax.sharding import PartitionSpec as P

highest = lax.Precision.HIGHEST
inverse_temp = 40.0
LANES = 128
NN = (((1,), (0,)), ((), ()))
NT = (((1,), (1,)), ((), ()))


def tail_weight(count):
    total = 0.0
    for number in range(count):
        total += (inverse_temp / (math.pi * (2 * number + 1))) ** 2
    return inverse_temp / 4.0 - 2.0 / inverse_temp * total


def dot(a, b, dims, precision=highest):
    return lax.dot_general(a, b, dims, precision=precision, preferred_element_type=jnp.float32)


def split(x):
    high = x.astype(jnp.bfloat16)
    return high, (x - high.astype(jnp.float32)).astype(jnp.bfloat16)


def dot3(a, b, dims):
    return sum(
        lax.dot_general(x, y, dims, preferred_element_type=jnp.float32)
        for x, y in ((a[0], b[0]), (a[0], b[1]), (a[1], b[0]))
    )


def iota(shape, dim):
    return lax.broadcasted_iota(jnp.int32, shape, dim)


def matsubara(number):
    return (2.0 * number.astype(jnp.float32) + 1.0) * (math.pi / inverse_temp)


def spare_of(norb):
    used = norb * norb
    width = LANES - used
    pieces = -(-used // width)
    return used, width, pieces


def kept_rows(norb, rows):
    pieces = spare_of(norb)[2]
    extra = 0
    while pieces * (extra + 1) <= rows - (extra + 1):
        extra += 1
    return rows - extra


def pack(rows, norb):
    used, width, pieces = spare_of(norb)
    kept = kept_rows(norb, len(rows))
    out = list(rows[:kept])
    lane = iota(rows[0].shape, 1)
    for e, row in enumerate(rows[kept:]):
        for p in range(pieces):
            moved = pltpu.roll(row, (used - width * p) % LANES, 1)
            out[pieces * e + p] = jnp.where(lane < used, out[pieces * e + p], moved)
    return out


def unpack(kept, norb, rows):
    used, width, pieces = spare_of(norb)
    out = list(kept)
    lane = iota(kept[0].shape, 1)
    for e in range(rows - len(kept)):
        row = 0.0
        for p in range(pieces):
            moved = pltpu.roll(kept[pieces * e + p], (width * p - used) % LANES, 1)
            inside = (lane >= width * p) & (lane < min(width * (p + 1), used))
            row = jnp.where(inside, moved, row)
        out.append(row)
    return out


def spaced(ref, chips, norb, rows):
    pitch = kept_rows(norb, rows)
    return unpack([ref[pl.ds(r, chips, stride=pitch), :] for r in range(pitch)], norb, rows)


def upright(rows):
    return jnp.concatenate(rows, axis=0).T


def invert(mat_re, mat_im):
    size = len(mat_re)
    mat_re, mat_im = list(mat_re), list(mat_im)
    column = iota(mat_re[0].shape, 0)
    for p in range(size):
        at = column == p
        piv_re = mat_re[p][p : p + 1]
        piv_im = mat_im[p][p : p + 1]
        rec = 1.0 / (piv_re * piv_re + piv_im * piv_im)
        rec_re = piv_re * rec
        rec_im = -piv_im * rec
        old_re = jnp.where(at, 1.0, mat_re[p])
        old_im = jnp.where(at, 0.0, mat_im[p])
        row_re = old_re * rec_re - old_im * rec_im
        row_im = old_re * rec_im + old_im * rec_re
        for i in range(size):
            if i == p:
                continue
            col_re = mat_re[i][p : p + 1]
            col_im = mat_im[i][p : p + 1]
            rest_re = jnp.where(at, 0.0, mat_re[i])
            rest_im = jnp.where(at, 0.0, mat_im[i])
            mat_re[i] = rest_re - (col_re * row_re - col_im * row_im)
            mat_im[i] = rest_im - (col_re * row_im + col_im * row_re)
        mat_re[p] = row_re
        mat_im[p] = row_im
    return mat_re, mat_im


def rows_of(block, norb):
    return [block[norb * i : norb * (i + 1)] for i in range(norb)]


def fetched(sources, targets, sems):
    copies = [pltpu.make_async_copy(a, b, sems.at[k]) for k, (a, b) in enumerate(zip(sources, targets))]
    for copy in copies:
        copy.start()

    def wait():
        for copy in copies:
            copy.wait()

    return wait


def band_inside(shape, window_ref):
    band = iota(shape, 1)
    return (band >= window_ref[:, 0:1]) & (band < window_ref[:, 1:2])


def project_kernel(
    norb, chips, freqs, core_axis, energy_in, proj_in, window_in, packed_ref, plain_ref,
    energy_ref, proj_ref, window_ref, flat_ref, sems,
):
    wait = fetched((energy_in, proj_in, window_in), (energy_ref, proj_ref, window_ref), sems)
    core = lax.axis_index(core_axis)
    bands = energy_ref.shape[1]
    rows = freqs * chips
    flat_ref[...] = jnp.zeros_like(flat_ref)
    freq = matsubara(numbers_down((2 * rows, bands), chips, freqs, core))
    square = freq * freq
    pair = iota((flat_ref.shape[0], LANES), 1)
    orb = iota((flat_ref.shape[0], LANES), 0)
    first = sum((pair >= norb * t).astype(jnp.int32) for t in range(1, norb))
    second = pair - norb * first
    inside = pair < norb * norb
    picks = [
        jnp.where((2 * which + half == orb) & inside, 1.0, 0.0)
        for which in (first, second)
        for half in range(2)
    ]
    picks = jnp.concatenate(picks, axis=1)
    wait()
    for i in range(norb):
        flat_ref[2 * i : 2 * i + 2, :bands] = proj_ref[0, i]
    flat = jnp.where(band_inside(flat_ref.shape, window_ref), flat_ref[...], 0.0)
    picked = dot(flat, picks, (((0,), (0,)), ((), ())))
    i_re, i_im, j_re, j_im = (picked[:, LANES * k : LANES * (k + 1)] for k in range(4))
    pair_re = (i_re * j_re + i_im * j_im)[:bands]
    pair_im = (i_im * j_re - i_re * j_im)[:bands]
    energy = energy_ref[...]
    denom = 1.0 / (energy * energy + square)
    both = dot(-energy * denom, jnp.concatenate([pair_re, pair_im], axis=1), NN) + dot(
        freq * denom, jnp.concatenate([pair_im, -pair_re], axis=1), NN
    )
    lines = []
    for other in range(2):
        for half in range(2):
            total = both[rows * other : rows * (other + 1), LANES * half : LANES * (half + 1)]
            at = rows * (len(lines) // freqs)
            plain_ref[at : at + rows, :] = total
            lines += [total[chips * f : chips * (f + 1)] for f in range(freqs)]
    lines = pack(lines, norb)
    for r, line in enumerate(lines):
        packed_ref[pl.ds(r, chips, stride=len(lines)), :] = line


def dyson_kernel(
    norb, chips, freqs, points, own_ref, sib_ref, wide_ref, new_ref, tile_ref,
    mat_ref, turn_ref,
):
    pairs = norb * norb
    group = 2 * freqs
    lines = spaced(own_ref, chips, norb, 2 * group)[:group]
    lines += spaced(sib_ref, chips, norb, 2 * group)[group:]
    for half in range(2):
        for part in range(2):
            at = group * part + freqs * half
            mat_ref[half, :, LANES * part : LANES * (part + 1)] = upright(lines[at : at + freqs])
    def rows(ref, base):
        return [ref[base + norb * i : base + norb * (i + 1), :] for i in range(norb)]

    sig_re, sig_im = rows(wide_ref, 0), rows(wide_ref, pairs)
    for part in range(2):
        lanes = pl.ds(LANES * part, LANES)
        mat = [
            [mat_ref[half, norb * i : norb * (i + 1), lanes] for i in range(norb)]
            for half in range(2)
        ]
        ainv_re, ainv_im = invert(*mat)
        gorb_re, gorb_im = invert(
            [a - s for a, s in zip(ainv_re, sig_re)], [a - s for a, s in zip(ainv_im, sig_im)]
        )
        sums = [a + b for a, b in zip(sums, gorb_re + gorb_im)] if part else gorb_re + gorb_im
    shift = chips // 2
    while shift:
        sums = [a + pltpu.roll(a, LANES - shift, 1) for a in sums]
        shift //= 2
    sums = [a * (1.0 / points) for a in sums]
    inv = invert(sums[:norb], sums[norb:])
    imp = rows(wide_ref, 2 * pairs), rows(wide_ref, 3 * pairs)
    pitch = turn_ref.shape[1] // norb
    diff = [[v - m for v, m in zip(inv[half], imp[half])] for half in range(2)]
    for half in range(2):
        for i in range(norb):
            turn_ref[half, pitch * i : pitch * i + norb, :] = diff[half][i]
    mat_ref[...] = jnp.zeros_like(mat_ref)
    for half, sig, sign in ((0, sig_re, 1.0), (1, sig_im, -1.0)):
        for i in range(norb):
            across = turn_ref[half, pl.ds(i, norb, stride=pitch), :]
            fresh = sig[i] + 0.5 * (diff[half][i] + sign * across)
            mat_ref[half, norb * i : norb * (i + 1), :LANES] = fresh
    lines = []
    for half in range(2):
        flipped = mat_ref[half, :, :LANES].T
        lines += [flipped[chips * f : chips * f + 1] for f in range(freqs)]
    tile = jnp.concatenate(lines, axis=0)
    for half in range(2):
        for i in range(norb):
            new_ref[half, i] = tile[freqs * half : freqs * (half + 1), norb * i : norb * (i + 1)]
    lines = pack(lines, norb)
    for r, line in enumerate(lines):
        tile_ref[pl.ds(r, chips, stride=len(lines)), :] = jnp.broadcast_to(line, (chips, LANES))


def numbers_down(shape, chips, freqs, core):
    row = iota(shape, 0)
    part = row // LANES
    within = row - LANES * part
    place = within // chips
    return 2 * freqs * (within - chips * place) + freqs * (core ^ part) + place


def numbers(shape, chips, freqs, core):
    lane = iota(shape, 1)
    part = lane // LANES
    within = lane - LANES * part
    place = within // chips
    return 2 * freqs * (within - chips * place) + freqs * (core ^ part) + place


STEP = 16


def prepare_kernel(
    norb, chips, freqs, core_axis, energy_in, proj_in, window_in, sigma_ref, imp_ref, plain_ref,
    ainv_ref, green_ref, left_ref, side_ref, right_ref, wide_ref,
    energy_ref, proj_ref, window_ref, flat_ref, small_ref, sems,
):
    wait = fetched((energy_in, proj_in, window_in), (energy_ref, proj_ref, window_ref), sems)
    core = lax.axis_index(core_axis)
    pairs = norb * norb
    for which, ref in enumerate((sigma_ref, imp_ref)):
        for half in range(2):
            for i in range(norb):
                at = (which * 2 + half) * pairs + norb * i
                small_ref[at : at + norb, :] = ref[half, i]
    spread = jnp.where(iota((freqs, LANES), 1) // chips == iota((freqs, LANES), 0), 1.0, 0.0)
    wide_ref[...] = dot(small_ref[...], spread, NN)
    bands = energy_ref.shape[1]
    tall = green_ref.shape[1]
    count = green_ref.shape[2]
    rows = freqs * chips
    for part in range(2):
        mat = []
        for half in range(2):
            at = rows * (2 * part + half)
            turned = plain_ref[at : at + rows, :].T
            mat.append(rows_of(turned, norb))
        inv = invert(*mat)
        for half in range(2):
            for i in range(norb):
                ainv_ref[2 * half + part, norb * i : norb * (i + 1), :] = inv[half][i]

    flat_ref[...] = jnp.zeros_like(flat_ref)
    wait()
    for i in range(norb):
        flat_ref[i : i + 1, :bands] = proj_ref[0, i, 0:1]
        flat_ref[STEP + i : STEP + i + 1, :bands] = proj_ref[0, i, 1:2]
    flat_ref[2 * STEP : 2 * STEP + 1, :bands] = energy_ref[...]
    keep = band_inside(flat_ref.shape, window_ref) | (iota(flat_ref.shape, 0) >= 2 * STEP)
    turned = jnp.where(keep, flat_ref[...], 0.0).T[:tall]
    energy = turned[:, 2 * STEP : 2 * STEP + 1]
    freq = matsubara(numbers((tall, count), chips, freqs, core))
    denom = 1.0 / (energy * energy + freq * freq)
    green_re = -energy * denom
    green_im = -freq * denom
    green_ref[0] = green_re
    green_ref[1] = green_im
    wide = 2 * STEP
    straight = turned[:, :wide]
    high, low = split(straight)
    left_ref[...] = jnp.concatenate([high, high, low], axis=1)
    flat = jnp.where(keep, flat_ref[...], 0.0)
    span = flat.shape[1]
    energy = flat[2 * STEP : 2 * STEP + 1]
    freq = matsubara(numbers_down((count, span), chips, freqs, core))
    denom = 1.0 / (energy * energy + freq * freq)
    green_re = -energy * denom
    green_im = -freq * denom
    for j in range(norb):
        p_re = flat[j : j + 1]
        p_im = flat[STEP + j : STEP + j + 1]
        re = split(green_re * p_re - green_im * p_im)
        im = split(green_re * p_im + green_im * p_re)
        for k in range(2):
            right_ref[j, k, :, :span] = re[k]
            right_ref[j, k, :, span:] = im[k]
    side_ref[...] = jnp.zeros_like(side_ref)
    side_ref[:norb, :span] = flat[:norb]
    side_ref[:norb, span:] = flat[STEP : STEP + norb]


def solve(mat, rhs):
    size = len(mat[0])
    mat = [list(m) for m in mat]
    out = [list(r) for r in rhs]
    row = iota(mat[0][0].shape, 0)
    for p in range(size):
        at = row == p
        piv_re = mat[0][p][p : p + 1]
        piv_im = mat[1][p][p : p + 1]
        rec = 1.0 / (piv_re * piv_re + piv_im * piv_im)
        rec_re = piv_re * rec
        rec_im = -piv_im * rec
        old_re = jnp.where(at, -1.0, mat[0][p])
        old_im = jnp.where(at, 0.0, mat[1][p])
        col_re = old_re * rec_re - old_im * rec_im
        col_im = old_re * rec_im + old_im * rec_re
        for cols, start in ((mat, p + 1), (out, 0)):
            for q in range(start, size):
                x_re = cols[0][q][p : p + 1]
                x_im = cols[1][q][p : p + 1]
                rest_re = jnp.where(at, 0.0, cols[0][q])
                rest_im = jnp.where(at, 0.0, cols[1][q])
                cols[0][q] = rest_re - (col_re * x_re - col_im * x_im)
                cols[1][q] = rest_im - (col_re * x_im + col_im * x_re)
    return out


def density_kernel(
    norb, chips, freqs, core_axis, ainv_ref, green_ref, left_ref, side_ref, right_ref, own_ref, sib_ref,
    out_ref, sig_ref, vert_ref, sums_ref, held_ref, done,
):
    core = lax.axis_index(core_axis)
    fetches = [
        pltpu.make_async_copy(right_ref.at[j], held_ref.at[j], done.at[j]) for j in range(norb)
    ]
    for fetch in fetches:
        fetch.start()
    group = 2 * freqs
    bands = out_ref.shape[2]
    tall = green_ref.shape[1]
    count = green_ref.shape[2]
    wide = 2 * STEP
    for part in range(2):
        lines = spaced((own_ref, sib_ref)[part], chips, norb, group)
        for half in range(2):
            sig_ref[2 * half + part] = upright(lines[freqs * half : freqs * (half + 1)])

    def columns(ref, half, part):
        return [ref[2 * half + part, pl.ds(j, norb, stride=norb), :] for j in range(norb)]

    spare = jnp.zeros((STEP - norb, 2 * norb * count), jnp.float32)
    vert_ref[norb:STEP] = spare
    vert_ref[STEP + norb : wide] = spare
    for part in range(2):
        sig = [columns(sig_ref, half, part) for half in range(2)]
        mat = [
            [a - s for a, s in zip(columns(ainv_ref, half, part), sig[half])] for half in range(2)
        ]
        turned = solve(mat, sig)
        for j in range(norb):
            sum_re, sum_im = sig[0][j], sig[1][j]
            for k in range(norb):
                y_re = turned[0][j][k : k + 1]
                y_im = turned[1][j][k : k + 1]
                sum_re = sum_re + (sig[0][k] * y_re - sig[1][k] * y_im)
                sum_im = sum_im + (sig[0][k] * y_im + sig[1][k] * y_re)
            at = 2 * count * j + LANES * part
            vert_ref[0:norb, at : at + LANES] = sum_re
            vert_ref[STEP : STEP + norb, at : at + LANES] = sum_im
            at += count
            vert_ref[0:norb, at : at + LANES] = sum_im
            vert_ref[STEP : STEP + norb, at : at + LANES] = -sum_re

    last = numbers((norb, count), chips, freqs, core) == count - 1
    orb = iota((norb, LANES), 1)
    ends = []
    for half in range(2):
        end = jnp.zeros((norb, LANES), jnp.float32)
        for j in range(norb):
            for part in range(2):
                spot = last[:, LANES * part : LANES * (part + 1)]
                entry = jnp.where(spot, columns(sig_ref, half, part)[j], 0.0)
                end = end + jnp.where(orb == j, jnp.sum(entry, axis=1, keepdims=True), 0.0)
        ends.append(end)
    blank = jnp.zeros((STEP - norb, LANES), jnp.float32)
    ends = [
        jnp.concatenate([a, blank, b, blank], axis=0) for a, b in (ends, (ends[1], -ends[0]))
    ]
    left = left_ref[...]

    def mixed(block):
        high, low = split(block)
        stacked = jnp.concatenate([high, low, high], axis=0)
        return lax.dot_general(left, stacked, NN, preferred_element_type=jnp.float32)

    def join(re, im, right):
        size = right[0].shape[1] // 2
        left = [jnp.concatenate([r, i], axis=1) for r, i in zip(split(re), split(im))]
        turned = [jnp.concatenate([-h[:, size:], h[:, :size]], axis=1) for h in right]
        return dot3(left, [jnp.concatenate([a, b], axis=0) for a, b in zip(right, turned)], NN)

    weight = -0.5 * inverse_temp * tail_weight(count)
    tail = weight * mixed(jnp.concatenate(ends, axis=1))
    total = join(tail[:, :LANES], tail[:, LANES:], split(side_ref[...]))
    green_re, green_im = green_ref[0], green_ref[1]
    for j in range(norb):
        mix = mixed(vert_ref[:, 2 * count * j : 2 * count * (j + 1)])
        mix_re, mix_im = mix[:, :count], mix[:, count:]
        side_re = mix_re * green_re - mix_im * green_im
        side_im = mix_re * green_im + mix_im * green_re
        fetches[j].wait()
        total = total + join(side_re, side_im, [held_ref[j, k] for k in range(2)])
    span = sums_ref.shape[1]
    sums_ref[...] = jnp.zeros_like(sums_ref)
    for half, sign in ((0, 1.0), (1, -1.0)):
        sums_ref[:tall, :] = total[:, span * half : span * (half + 1)]
        both = sums_ref[...] + sign * sums_ref[...].T
        out_ref[0, half] = both[:bands, :bands] / inverse_temp


HBM = pl.BlockSpec(memory_space=pltpu.HBM)
VMEM = pl.BlockSpec(memory_space=pltpu.VMEM)


def struct(*shape, dtype=jnp.float32):
    return jax.ShapeDtypeStruct(shape, dtype)


def scratch(*shape):
    return pltpu.VMEM(shape, jnp.float32)


def run(body, out, specs, scratches=()):
    return pl.pallas_call(
        body,
        out_shape=out,
        in_specs=specs,
        out_specs=jax.tree.map(lambda _: VMEM, out),
        scratch_shapes=scratches,
        compiler_params=pltpu.CompilerParams(vmem_limit_bytes=32 * 1024 * 1024),
    )


def kernels(norb, bands, freqs, chips, cores, points):
    group = 2 * freqs
    pairs = norb * norb
    count = freqs * chips * cores
    wide = -(-bands // LANES) * LANES
    tall = -(-bands // 16) * 16
    long = kept_rows(norb, 2 * group)
    short = kept_rows(norb, group)
    axis = "core"

    def project(*refs):
        project_kernel(norb, chips, freqs, axis, *refs)

    def dyson(*refs):
        dyson_kernel(norb, chips, freqs, points, *refs)

    def prepare(*refs):
        prepare_kernel(norb, chips, freqs, axis, *refs)

    def rebuild(*refs):
        density_kernel(norb, chips, freqs, axis, *refs)

    inputs = [
        pltpu.VMEM((1, bands), jnp.float32),
        pltpu.VMEM((1, norb, 2, bands), jnp.float32),
        pltpu.VMEM((1, 2), jnp.int32),
    ]
    first = run(
        project,
        (struct(chips * long, LANES), struct(2 * count, LANES)),
        [HBM] * 3,
        [*inputs, scratch(24, wide), pltpu.SemaphoreType.DMA((3,))],
    )
    second = run(
        dyson,
        (struct(2, norb, freqs, norb), struct(chips * short, LANES)),
        [VMEM] * 3,
        [scratch(2, LANES, 2 * LANES), scratch(2, 16 * norb, LANES)],
    )
    aside = run(
        prepare,
        (
            struct(4, pairs, LANES),
            struct(2, tall, count),
            struct(tall, 6 * STEP, dtype=jnp.bfloat16),
            struct(LANES, 2 * wide),
            struct(norb, 2, count, 2 * wide, dtype=jnp.bfloat16),
            struct(4 * pairs, LANES),
        ),
        [HBM] * 3 + [VMEM] * 3,
        [
            *inputs,
            scratch(LANES, wide),
            scratch(4 * pairs, freqs),
            pltpu.SemaphoreType.DMA((3,)),
        ],
    )
    third = run(
        rebuild,
        struct(1, 2, bands, bands),
        [VMEM] * 4 + [HBM] + [VMEM] * 2,
        [
            scratch(4, LANES, LANES),
            scratch(2 * STEP, 2 * norb * count),
            scratch(wide, wide),
            pltpu.VMEM((norb, 2, count, 2 * wide), jnp.bfloat16),
            pltpu.SemaphoreType.DMA((norb,)),
        ],
    )
    return first, aside, second, third


def local(energies, proj, window, sigma, impurity_inverse):
    norb, bands = proj.shape[2:]
    freqs = sigma.shape[3]
    chips = lax.axis_size("z")
    cores = lax.axis_size("core")
    points = energies.shape[0] * chips * cores
    first, aside, second, third = kernels(norb, bands, freqs, chips, cores, points)
    swap = [(0, 1), (1, 0)]
    proj = jnp.swapaxes(proj, 1, 2)

    def across(rows):
        got = lax.all_to_all(rows.reshape(chips, 1, -1), "z", 0, 0, tiled=True)
        return got.reshape(rows.shape)

    far = [pltpu.with_memory_space_constraint(x, pltpu.HBM) for x in (energies, proj, window)]
    packed, plain = first(*far)
    ready = aside(*far, sigma, impurity_inverse, plain)
    got, ready = lax.optimization_barrier((across(packed), ready))
    *ready, spread = ready
    sigma_new, tiles = second(got, lax.ppermute(got, "core", swap), spread)
    back = across(tiles)
    ready[4] = pltpu.with_memory_space_constraint(ready[4], pltpu.HBM)
    density = third(*ready, back, lax.ppermute(back, "core", swap))
    return density, jnp.swapaxes(sigma_new, 2, 3)


def solution(mesh):
    parts, line = mesh.shape["parts"], mesh.shape["ka"]
    torus = Mesh(mesh.devices.reshape(parts, line // 2, 2), ("parts", "z", "core"))
    every = ("parts", "z", "core")
    line = ("z", "core")
    in_specs = (
        P(every, None),
        P(every, None, None, None),
        P(every, None),
        P("parts", None, None, line),
        P("parts", None, None, line),
    )
    out_specs = (P(every, None, None, None), P("parts", None, None, line))
    return jax.shard_map(local, mesh=torus, in_specs=in_specs, out_specs=out_specs, check_vma=False)
```

```python
import math

import jax
import jax.numpy as jnp
from jax import lax
from jax.experimental import pallas as pl
from jax.experimental.pallas import tpu as pltpu
from jax.sharding import Mesh
from jax.sharding import PartitionSpec as P

highest = lax.Precision.HIGHEST
inverse_temp = 40.0
LANES = 128
NN = (((1,), (0,)), ((), ()))
NT = (((1,), (1,)), ((), ()))


def tail_weight(count):
    total = 0.0
    for number in range(count):
        total += (inverse_temp / (math.pi * (2 * number + 1))) ** 2
    return inverse_temp / 4.0 - 2.0 / inverse_temp * total


def dot(a, b, dims, precision=highest):
    return lax.dot_general(a, b, dims, precision=precision, preferred_element_type=jnp.float32)


def split(x):
    high = x.astype(jnp.bfloat16)
    return high, (x - high.astype(jnp.float32)).astype(jnp.bfloat16)


def dot3(a, b, dims):
    return sum(
        lax.dot_general(x, y, dims, preferred_element_type=jnp.float32)
        for x, y in ((a[0], b[0]), (a[0], b[1]), (a[1], b[0]))
    )


def iota(shape, dim):
    return lax.broadcasted_iota(jnp.int32, shape, dim)


def matsubara(number):
    return (2.0 * number.astype(jnp.float32) + 1.0) * (math.pi / inverse_temp)


def spare_of(norb):
    used = norb * norb
    width = LANES - used
    pieces = -(-used // width)
    return used, width, pieces


def kept_rows(norb, rows):
    pieces = spare_of(norb)[2]
    extra = 0
    while pieces * (extra + 1) <= rows - (extra + 1):
        extra += 1
    return rows - extra


def pack(rows, norb):
    used, width, pieces = spare_of(norb)
    kept = kept_rows(norb, len(rows))
    out = list(rows[:kept])
    lane = iota(rows[0].shape, 1)
    for e, row in enumerate(rows[kept:]):
        for p in range(pieces):
            moved = pltpu.roll(row, (used - width * p) % LANES, 1)
            out[pieces * e + p] = jnp.where(lane < used, out[pieces * e + p], moved)
    return out


def unpack(kept, norb, rows):
    used, width, pieces = spare_of(norb)
    out = list(kept)
    lane = iota(kept[0].shape, 1)
    for e in range(rows - len(kept)):
        row = 0.0
        for p in range(pieces):
            moved = pltpu.roll(kept[pieces * e + p], (width * p - used) % LANES, 1)
            inside = (lane >= width * p) & (lane < min(width * (p + 1), used))
            row = jnp.where(inside, moved, row)
        out.append(row)
    return out


def spaced(ref, chips, norb, rows):
    pitch = kept_rows(norb, rows)
    return unpack([ref[pl.ds(r, chips, stride=pitch), :] for r in range(pitch)], norb, rows)


def upright(rows):
    return jnp.concatenate(rows, axis=0).T


def invert(mat_re, mat_im):
    size = len(mat_re)
    mat_re, mat_im = list(mat_re), list(mat_im)
    column = iota(mat_re[0].shape, 0)
    for p in range(size):
        at = column == p
        piv_re = mat_re[p][p : p + 1]
        piv_im = mat_im[p][p : p + 1]
        rec = 1.0 / (piv_re * piv_re + piv_im * piv_im)
        rec_re = piv_re * rec
        rec_im = -piv_im * rec
        old_re = jnp.where(at, 1.0, mat_re[p])
        old_im = jnp.where(at, 0.0, mat_im[p])
        row_re = old_re * rec_re - old_im * rec_im
        row_im = old_re * rec_im + old_im * rec_re
        for i in range(size):
            if i == p:
                continue
            col_re = mat_re[i][p : p + 1]
            col_im = mat_im[i][p : p + 1]
            rest_re = jnp.where(at, 0.0, mat_re[i])
            rest_im = jnp.where(at, 0.0, mat_im[i])
            mat_re[i] = rest_re - (col_re * row_re - col_im * row_im)
            mat_im[i] = rest_im - (col_re * row_im + col_im * row_re)
        mat_re[p] = row_re
        mat_im[p] = row_im
    return mat_re, mat_im


def rows_of(block, norb):
    return [block[norb * i : norb * (i + 1)] for i in range(norb)]


def fetched(sources, targets, sems):
    copies = [pltpu.make_async_copy(a, b, sems.at[k]) for k, (a, b) in enumerate(zip(sources, targets))]
    for copy in copies:
        copy.start()

    def wait():
        for copy in copies:
            copy.wait()

    return wait


def band_inside(shape, window_ref):
    band = iota(shape, 1)
    return (band >= window_ref[:, 0:1]) & (band < window_ref[:, 1:2])


def project_kernel(
    norb, chips, freqs, core_axis, energy_in, proj_in, window_in, packed_ref, plain_ref,
    energy_ref, proj_ref, window_ref, flat_ref, sems,
):
    wait = fetched((energy_in, proj_in, window_in), (energy_ref, proj_ref, window_ref), sems)
    core = lax.axis_index(core_axis)
    bands = energy_ref.shape[1]
    rows = freqs * chips
    flat_ref[...] = jnp.zeros_like(flat_ref)
    freq = matsubara(numbers((2 * rows, bands), 0, chips, 1, freqs, core))
    square = freq * freq
    pair = iota((flat_ref.shape[0], LANES), 1)
    orb = iota((flat_ref.shape[0], LANES), 0)
    first = sum((pair >= norb * t).astype(jnp.int32) for t in range(1, norb))
    second = pair - norb * first
    inside = pair < norb * norb
    picks = [
        jnp.where((2 * which + half == orb) & inside, 1.0, 0.0)
        for which in (first, second)
        for half in range(2)
    ]
    picks = jnp.concatenate(picks, axis=1)
    wait()
    for i in range(norb):
        flat_ref[2 * i : 2 * i + 2, :bands] = proj_ref[0, i]
    flat = jnp.where(band_inside(flat_ref.shape, window_ref), flat_ref[...], 0.0)
    picked = dot(flat, picks, (((0,), (0,)), ((), ())))
    i_re, i_im, j_re, j_im = (picked[:, LANES * k : LANES * (k + 1)] for k in range(4))
    pair_re = (i_re * j_re + i_im * j_im)[:bands]
    pair_im = (i_im * j_re - i_re * j_im)[:bands]
    energy = energy_ref[...]
    denom = 1.0 / (energy * energy + square)
    both = dot(-energy * denom, jnp.concatenate([pair_re, pair_im], axis=1), NN) + dot(
        freq * denom, jnp.concatenate([pair_im, -pair_re], axis=1), NN
    )
    lines = []
    for other in range(2):
        for half in range(2):
            total = both[rows * other : rows * (other + 1), LANES * half : LANES * (half + 1)]
            at = rows * (len(lines) // freqs)
            plain_ref[at : at + rows, :] = total
            lines += [total[chips * f : chips * (f + 1)] for f in range(freqs)]
    lines = pack(lines, norb)
    for r, line in enumerate(lines):
        packed_ref[pl.ds(r, chips, stride=len(lines)), :] = line


def dyson_kernel(
    norb, chips, freqs, points, own_ref, sib_ref, wide_ref, new_ref, tile_ref,
    mat_ref, turn_ref,
):
    pairs = norb * norb
    group = 2 * freqs
    lines = spaced(own_ref, chips, norb, 2 * group)[:group]
    lines += spaced(sib_ref, chips, norb, 2 * group)[group:]
    for half in range(2):
        for part in range(2):
            at = group * part + freqs * half
            mat_ref[half, :, LANES * part : LANES * (part + 1)] = upright(lines[at : at + freqs])
    def rows(ref, base):
        return [ref[base + norb * i : base + norb * (i + 1), :] for i in range(norb)]

    sig_re, sig_im = rows(wide_ref, 0), rows(wide_ref, pairs)
    for part in range(2):
        lanes = pl.ds(LANES * part, LANES)
        mat = [
            [mat_ref[half, norb * i : norb * (i + 1), lanes] for i in range(norb)]
            for half in range(2)
        ]
        ainv_re, ainv_im = invert(*mat)
        gorb_re, gorb_im = invert(
            [a - s for a, s in zip(ainv_re, sig_re)], [a - s for a, s in zip(ainv_im, sig_im)]
        )
        sums = [a + b for a, b in zip(sums, gorb_re + gorb_im)] if part else gorb_re + gorb_im
    shift = chips // 2
    while shift:
        sums = [a + pltpu.roll(a, LANES - shift, 1) for a in sums]
        shift //= 2
    sums = [a * (1.0 / points) for a in sums]
    inv = invert(sums[:norb], sums[norb:])
    imp = rows(wide_ref, 2 * pairs), rows(wide_ref, 3 * pairs)
    pitch = turn_ref.shape[1] // norb
    diff = [[v - m for v, m in zip(inv[half], imp[half])] for half in range(2)]
    for half in range(2):
        for i in range(norb):
            turn_ref[half, pitch * i : pitch * i + norb, :] = diff[half][i]
    mat_ref[...] = jnp.zeros_like(mat_ref)
    for half, sig, sign in ((0, sig_re, 1.0), (1, sig_im, -1.0)):
        for i in range(norb):
            across = turn_ref[half, pl.ds(i, norb, stride=pitch), :]
            fresh = sig[i] + 0.5 * (diff[half][i] + sign * across)
            mat_ref[half, norb * i : norb * (i + 1), :LANES] = fresh
    lines = []
    for half in range(2):
        flipped = mat_ref[half, :, :LANES].T
        lines += [flipped[chips * f : chips * f + 1] for f in range(freqs)]
    tile = jnp.concatenate(lines, axis=0)
    for half in range(2):
        for i in range(norb):
            new_ref[half, i] = tile[freqs * half : freqs * (half + 1), norb * i : norb * (i + 1)]
    lines = pack(lines, norb)
    for r, line in enumerate(lines):
        tile_ref[0, :, LANES * r : LANES * (r + 1)] = line


def numbers(shape, dim, chips, near, freqs, core):
    spot = iota(shape, dim)
    part = spot // LANES
    within = spot - LANES * part
    place = within // chips
    chip = within - chips * place
    far = chips // near
    close = chip // far
    chip = near * (chip - far * close) + close
    return 2 * freqs * chip + freqs * (core ^ part) + place


STEP = 16


def prepare_kernel(
    norb, chips, near, freqs, core_axis, energy_in, proj_in, window_in, sigma_ref, imp_ref, plain_ref,
    ainv_ref, green_ref, left_ref, side_ref, right_ref, wide_ref,
    energy_ref, proj_ref, window_ref, flat_ref, small_ref, sems,
):
    wait = fetched((energy_in, proj_in, window_in), (energy_ref, proj_ref, window_ref), sems)
    core = lax.axis_index(core_axis)
    pairs = norb * norb
    for which, ref in enumerate((sigma_ref, imp_ref)):
        for half in range(2):
            for i in range(norb):
                at = (which * 2 + half) * pairs + norb * i
                small_ref[at : at + norb, :] = ref[half, i]
    spread = jnp.where(iota((freqs, LANES), 1) // chips == iota((freqs, LANES), 0), 1.0, 0.0)
    wide_ref[...] = dot(small_ref[...], spread, NN)
    bands = energy_ref.shape[1]
    tall = green_ref.shape[1]
    count = green_ref.shape[2]
    rows = freqs * chips
    for part in range(2):
        mat = []
        for half in range(2):
            at = rows * (2 * part + half)
            order = [
                plain_ref[pl.ds(at + chips * f + close, chips // near, stride=near), :]
                for f in range(freqs)
                for close in range(near)
            ]
            mat.append(rows_of(upright(order), norb))
        inv = invert(*mat)
        for half in range(2):
            for i in range(norb):
                ainv_ref[2 * half + part, norb * i : norb * (i + 1), :] = inv[half][i]

    flat_ref[...] = jnp.zeros_like(flat_ref)
    wait()
    for i in range(norb):
        flat_ref[i : i + 1, :bands] = proj_ref[0, i, 0:1]
        flat_ref[STEP + i : STEP + i + 1, :bands] = proj_ref[0, i, 1:2]
    flat_ref[2 * STEP : 2 * STEP + 1, :bands] = energy_ref[...]
    keep = band_inside(flat_ref.shape, window_ref) | (iota(flat_ref.shape, 0) >= 2 * STEP)
    turned = jnp.where(keep, flat_ref[...], 0.0).T[:tall]
    energy = turned[:, 2 * STEP : 2 * STEP + 1]
    freq = matsubara(numbers((tall, count), 1, chips, near, freqs, core))
    denom = 1.0 / (energy * energy + freq * freq)
    green_re = -energy * denom
    green_im = -freq * denom
    green_ref[0] = green_re
    green_ref[1] = green_im
    wide = 2 * STEP
    straight = turned[:, :wide]
    high, low = split(straight)
    left_ref[...] = jnp.concatenate([high, high, low], axis=1)
    flat = jnp.where(keep, flat_ref[...], 0.0)
    span = flat.shape[1]
    energy = flat[2 * STEP : 2 * STEP + 1]
    freq = matsubara(numbers((count, span), 0, chips, near, freqs, core))
    denom = 1.0 / (energy * energy + freq * freq)
    green_re = -energy * denom
    green_im = -freq * denom
    for j in range(norb):
        p_re = flat[j : j + 1]
        p_im = flat[STEP + j : STEP + j + 1]
        re = split(green_re * p_re - green_im * p_im)
        im = split(green_re * p_im + green_im * p_re)
        for k in range(2):
            right_ref[j, k, :, :span] = re[k]
            right_ref[j, k, :, span:] = im[k]
    side_ref[...] = jnp.zeros_like(side_ref)
    side_ref[:norb, :span] = flat[:norb]
    side_ref[:norb, span:] = flat[STEP : STEP + norb]


def solve(mat, rhs):
    size = len(mat[0])
    mat = [list(m) for m in mat]
    out = [list(r) for r in rhs]
    row = iota(mat[0][0].shape, 0)
    for p in range(size):
        at = row == p
        piv_re = mat[0][p][p : p + 1]
        piv_im = mat[1][p][p : p + 1]
        rec = 1.0 / (piv_re * piv_re + piv_im * piv_im)
        rec_re = piv_re * rec
        rec_im = -piv_im * rec
        old_re = jnp.where(at, -1.0, mat[0][p])
        old_im = jnp.where(at, 0.0, mat[1][p])
        col_re = old_re * rec_re - old_im * rec_im
        col_im = old_re * rec_im + old_im * rec_re
        for cols, start in ((mat, p + 1), (out, 0)):
            for q in range(start, size):
                x_re = cols[0][q][p : p + 1]
                x_im = cols[1][q][p : p + 1]
                rest_re = jnp.where(at, 0.0, cols[0][q])
                rest_im = jnp.where(at, 0.0, cols[1][q])
                cols[0][q] = rest_re - (col_re * x_re - col_im * x_im)
                cols[1][q] = rest_im - (col_re * x_im + col_im * x_re)
    return out


def density_kernel(
    norb, chips, near, freqs, core_axis, ainv_ref, green_ref, left_ref, side_ref, right_ref, own_ref, sib_ref,
    out_ref, sig_ref, vert_ref, sums_ref, held_ref, done,
):
    core = lax.axis_index(core_axis)
    fetches = [
        pltpu.make_async_copy(right_ref.at[j], held_ref.at[j], done.at[j]) for j in range(norb)
    ]
    for fetch in fetches:
        fetch.start()
    group = 2 * freqs
    bands = out_ref.shape[2]
    tall = green_ref.shape[1]
    count = green_ref.shape[2]
    wide = 2 * STEP
    for part in range(2):
        lines = spaced((own_ref, sib_ref)[part], chips, norb, group)
        for half in range(2):
            sig_ref[2 * half + part] = upright(lines[freqs * half : freqs * (half + 1)])

    def columns(ref, half, part):
        return [ref[2 * half + part, pl.ds(j, norb, stride=norb), :] for j in range(norb)]

    spare = jnp.zeros((STEP - norb, 2 * norb * count), jnp.float32)
    vert_ref[norb:STEP] = spare
    vert_ref[STEP + norb : wide] = spare
    for part in range(2):
        sig = [columns(sig_ref, half, part) for half in range(2)]
        mat = [
            [a - s for a, s in zip(columns(ainv_ref, half, part), sig[half])] for half in range(2)
        ]
        turned = solve(mat, sig)
        for j in range(norb):
            sum_re, sum_im = sig[0][j], sig[1][j]
            for k in range(norb):
                y_re = turned[0][j][k : k + 1]
                y_im = turned[1][j][k : k + 1]
                sum_re = sum_re + (sig[0][k] * y_re - sig[1][k] * y_im)
                sum_im = sum_im + (sig[0][k] * y_im + sig[1][k] * y_re)
            at = 2 * count * j + LANES * part
            vert_ref[0:norb, at : at + LANES] = sum_re
            vert_ref[STEP : STEP + norb, at : at + LANES] = sum_im
            at += count
            vert_ref[0:norb, at : at + LANES] = sum_im
            vert_ref[STEP : STEP + norb, at : at + LANES] = -sum_re

    last = numbers((norb, count), 1, chips, near, freqs, core) == count - 1
    orb = iota((norb, LANES), 1)
    ends = []
    for half in range(2):
        end = jnp.zeros((norb, LANES), jnp.float32)
        for j in range(norb):
            for part in range(2):
                spot = last[:, LANES * part : LANES * (part + 1)]
                entry = jnp.where(spot, columns(sig_ref, half, part)[j], 0.0)
                end = end + jnp.where(orb == j, jnp.sum(entry, axis=1, keepdims=True), 0.0)
        ends.append(end)
    blank = jnp.zeros((STEP - norb, LANES), jnp.float32)
    ends = [
        jnp.concatenate([a, blank, b, blank], axis=0) for a, b in (ends, (ends[1], -ends[0]))
    ]
    left = left_ref[...]

    def mixed(block):
        high, low = split(block)
        stacked = jnp.concatenate([high, low, high], axis=0)
        return lax.dot_general(left, stacked, NN, preferred_element_type=jnp.float32)

    def join(re, im, right):
        size = right[0].shape[1] // 2
        left = [jnp.concatenate([r, i], axis=1) for r, i in zip(split(re), split(im))]
        turned = [jnp.concatenate([-h[:, size:], h[:, :size]], axis=1) for h in right]
        return dot3(left, [jnp.concatenate([a, b], axis=0) for a, b in zip(right, turned)], NN)

    weight = -0.5 * inverse_temp * tail_weight(count)
    tail = weight * mixed(jnp.concatenate(ends, axis=1))
    total = join(tail[:, :LANES], tail[:, LANES:], split(side_ref[...]))
    green_re, green_im = green_ref[0], green_ref[1]
    for j in range(norb):
        mix = mixed(vert_ref[:, 2 * count * j : 2 * count * (j + 1)])
        mix_re, mix_im = mix[:, :count], mix[:, count:]
        side_re = mix_re * green_re - mix_im * green_im
        side_im = mix_re * green_im + mix_im * green_re
        fetches[j].wait()
        total = total + join(side_re, side_im, [held_ref[j, k] for k in range(2)])
    span = sums_ref.shape[1]
    sums_ref[...] = jnp.zeros_like(sums_ref)
    for half, sign in ((0, 1.0), (1, -1.0)):
        sums_ref[:tall, :] = total[:, span * half : span * (half + 1)]
        both = sums_ref[...] + sign * sums_ref[...].T
        out_ref[0, half] = both[:bands, :bands] / inverse_temp


HBM = pl.BlockSpec(memory_space=pltpu.HBM)
VMEM = pl.BlockSpec(memory_space=pltpu.VMEM)


def struct(*shape, dtype=jnp.float32):
    return jax.ShapeDtypeStruct(shape, dtype)


def scratch(*shape):
    return pltpu.VMEM(shape, jnp.float32)


def run(body, out, specs, scratches=()):
    return pl.pallas_call(
        body,
        out_shape=out,
        in_specs=specs,
        out_specs=jax.tree.map(lambda _: VMEM, out),
        scratch_shapes=scratches,
        compiler_params=pltpu.CompilerParams(vmem_limit_bytes=32 * 1024 * 1024),
    )


def kernels(norb, bands, freqs, chips, near, cores, points):
    group = 2 * freqs
    pairs = norb * norb
    count = freqs * chips * cores
    wide = -(-bands // LANES) * LANES
    tall = -(-bands // 16) * 16
    long = kept_rows(norb, 2 * group)
    short = kept_rows(norb, group)
    axis = "core"

    def project(*refs):
        project_kernel(norb, chips, freqs, axis, *refs)

    def dyson(*refs):
        dyson_kernel(norb, chips, freqs, points, *refs)

    def prepare(*refs):
        prepare_kernel(norb, chips, near, freqs, axis, *refs)

    def rebuild(*refs):
        density_kernel(norb, chips, near, freqs, axis, *refs)

    inputs = [
        pltpu.VMEM((1, bands), jnp.float32),
        pltpu.VMEM((1, norb, 2, bands), jnp.float32),
        pltpu.VMEM((1, 2), jnp.int32),
    ]
    first = run(
        project,
        (struct(chips * long, LANES), struct(2 * count, LANES)),
        [HBM] * 3,
        [*inputs, scratch(24, wide), pltpu.SemaphoreType.DMA((3,))],
    )
    second = run(
        dyson,
        (struct(2, norb, freqs, norb), struct(1, 1, short * LANES)),
        [VMEM] * 3,
        [scratch(2, LANES, 2 * LANES), scratch(2, 16 * norb, LANES)],
    )
    aside = run(
        prepare,
        (
            struct(4, pairs, LANES),
            struct(2, tall, count),
            struct(tall, 6 * STEP, dtype=jnp.bfloat16),
            struct(LANES, 2 * wide),
            struct(norb, 2, count, 2 * wide, dtype=jnp.bfloat16),
            struct(4 * pairs, LANES),
        ),
        [HBM] * 3 + [VMEM] * 3,
        [
            *inputs,
            scratch(LANES, wide),
            scratch(4 * pairs, freqs),
            pltpu.SemaphoreType.DMA((3,)),
        ],
    )
    third = run(
        rebuild,
        struct(1, 2, bands, bands),
        [VMEM] * 4 + [HBM] + [VMEM] * 2,
        [
            scratch(4, LANES, LANES),
            scratch(2 * STEP, 2 * norb * count),
            scratch(wide, wide),
            pltpu.VMEM((norb, 2, count, 2 * wide), jnp.bfloat16),
            pltpu.SemaphoreType.DMA((norb,)),
        ],
    )
    return first, aside, second, third


def local(energies, proj, window, sigma, impurity_inverse):
    norb, bands = proj.shape[2:]
    freqs = sigma.shape[3]
    near = lax.axis_size("near")
    chips = lax.axis_size("far") * near
    cores = lax.axis_size("core")
    points = energies.shape[0] * chips * cores
    first, aside, second, third = kernels(norb, bands, freqs, chips, near, cores, points)
    swap = [(0, 1), (1, 0)]
    proj = jnp.swapaxes(proj, 1, 2)

    def across(rows):
        got = lax.all_to_all(rows.reshape(chips, 1, -1), ("far", "near"), 0, 0, tiled=True)
        return got.reshape(rows.shape)

    far = [pltpu.with_memory_space_constraint(x, pltpu.HBM) for x in (energies, proj, window)]
    packed, plain = first(*far)
    ready = aside(*far, sigma, impurity_inverse, plain)
    got, ready = lax.optimization_barrier((across(packed), ready))
    *ready, spread = ready
    sigma_new, tiles = second(got, lax.ppermute(got, "core", swap), spread)
    back = lax.all_gather(tiles, "far", axis=0, tiled=True)
    back = lax.all_gather(back, "near", axis=0, tiled=True).reshape(-1, LANES)
    ready[4] = pltpu.with_memory_space_constraint(ready[4], pltpu.HBM)
    density = third(*ready, back, lax.ppermute(back, "core", swap))
    return density, jnp.swapaxes(sigma_new, 2, 3)


def solution(mesh):
    parts, line = mesh.shape["parts"], mesh.shape["ka"]
    near = 4
    chips = line // 2
    torus = Mesh(
        mesh.devices.reshape(parts, chips // near, near, 2), ("parts", "far", "near", "core")
    )
    every = ("parts", "far", "near", "core")
    line = ("far", "near", "core")
    in_specs = (
        P(every, None),
        P(every, None, None, None),
        P(every, None),
        P("parts", None, None, line),
        P("parts", None, None, line),
    )
    out_specs = (P(every, None, None, None), P("parts", None, None, line))
    return jax.shard_map(local, mesh=torus, in_specs=in_specs, out_specs=out_specs, check_vma=False)
```

```python
import math

import jax
import jax.numpy as jnp
from jax import lax
from jax.experimental import pallas as pl
from jax.experimental.pallas import tpu as pltpu
from jax.sharding import Mesh
from jax.sharding import PartitionSpec as P

highest = lax.Precision.HIGHEST
inverse_temp = 40.0
LANES = 128
NN = (((1,), (0,)), ((), ()))
NT = (((1,), (1,)), ((), ()))


def tail_weight(count):
    total = 0.0
    for number in range(count):
        total += (inverse_temp / (math.pi * (2 * number + 1))) ** 2
    return inverse_temp / 4.0 - 2.0 / inverse_temp * total


def dot(a, b, dims, precision=highest):
    return lax.dot_general(a, b, dims, precision=precision, preferred_element_type=jnp.float32)


def split(x):
    high = x.astype(jnp.bfloat16)
    return high, (x - high.astype(jnp.float32)).astype(jnp.bfloat16)


def dot3(a, b, dims):
    return sum(
        lax.dot_general(x, y, dims, preferred_element_type=jnp.float32)
        for x, y in ((a[0], b[0]), (a[0], b[1]), (a[1], b[0]))
    )


def iota(shape, dim):
    return lax.broadcasted_iota(jnp.int32, shape, dim)


def matsubara(number):
    return (2.0 * number.astype(jnp.float32) + 1.0) * (math.pi / inverse_temp)


def spare_of(norb):
    used = norb * norb
    width = LANES - used
    pieces = -(-used // width)
    return used, width, pieces


def kept_rows(norb, rows):
    pieces = spare_of(norb)[2]
    extra = 0
    while pieces * (extra + 1) <= rows - (extra + 1):
        extra += 1
    return rows - extra


def pack(rows, norb):
    used, width, pieces = spare_of(norb)
    kept = kept_rows(norb, len(rows))
    out = list(rows[:kept])
    lane = iota(rows[0].shape, 1)
    for e, row in enumerate(rows[kept:]):
        for p in range(pieces):
            moved = pltpu.roll(row, (used - width * p) % LANES, 1)
            out[pieces * e + p] = jnp.where(lane < used, out[pieces * e + p], moved)
    return out


def unpack(kept, norb, rows):
    used, width, pieces = spare_of(norb)
    out = list(kept)
    lane = iota(kept[0].shape, 1)
    for e in range(rows - len(kept)):
        row = 0.0
        for p in range(pieces):
            moved = pltpu.roll(kept[pieces * e + p], (width * p - used) % LANES, 1)
            inside = (lane >= width * p) & (lane < min(width * (p + 1), used))
            row = jnp.where(inside, moved, row)
        out.append(row)
    return out


def spaced(ref, chips, norb, rows):
    pitch = kept_rows(norb, rows)
    return unpack([ref[pl.ds(r, chips, stride=pitch), :] for r in range(pitch)], norb, rows)


def upright(rows):
    return jnp.concatenate(rows, axis=0).T


def invert(mat_re, mat_im):
    size = len(mat_re)
    mat_re, mat_im = list(mat_re), list(mat_im)
    column = iota(mat_re[0].shape, 0)
    for p in range(size):
        at = column == p
        piv_re = mat_re[p][p : p + 1]
        piv_im = mat_im[p][p : p + 1]
        rec = 1.0 / (piv_re * piv_re + piv_im * piv_im)
        rec_re = piv_re * rec
        rec_im = -piv_im * rec
        old_re = jnp.where(at, 1.0, mat_re[p])
        old_im = jnp.where(at, 0.0, mat_im[p])
        row_re = old_re * rec_re - old_im * rec_im
        row_im = old_re * rec_im + old_im * rec_re
        for i in range(size):
            if i == p:
                continue
            col_re = mat_re[i][p : p + 1]
            col_im = mat_im[i][p : p + 1]
            rest_re = jnp.where(at, 0.0, mat_re[i])
            rest_im = jnp.where(at, 0.0, mat_im[i])
            mat_re[i] = rest_re - (col_re * row_re - col_im * row_im)
            mat_im[i] = rest_im - (col_re * row_im + col_im * row_re)
        mat_re[p] = row_re
        mat_im[p] = row_im
    return mat_re, mat_im


def rows_of(block, norb):
    return [block[norb * i : norb * (i + 1)] for i in range(norb)]


def fetched(sources, targets, sems):
    copies = [pltpu.make_async_copy(a, b, sems.at[k]) for k, (a, b) in enumerate(zip(sources, targets))]
    for copy in copies:
        copy.start()

    def wait():
        for copy in copies:
            copy.wait()

    return wait


def band_inside(shape, window_ref):
    band = iota(shape, 1)
    return (band >= window_ref[:, 0:1]) & (band < window_ref[:, 1:2])


def project_kernel(
    norb, chips, freqs, core_axis, energy_in, proj_in, window_in, packed_ref, plain_ref,
    energy_ref, proj_ref, window_ref, flat_ref, sems,
):
    wait = fetched((energy_in, proj_in, window_in), (energy_ref, proj_ref, window_ref), sems)
    core = lax.axis_index(core_axis)
    bands = energy_ref.shape[1]
    rows = freqs * chips
    flat_ref[...] = jnp.zeros_like(flat_ref)
    freq = matsubara(numbers_down((2 * rows, bands), chips, freqs, core))
    square = freq * freq
    pair = iota((flat_ref.shape[0], LANES), 1)
    orb = iota((flat_ref.shape[0], LANES), 0)
    first = sum((pair >= norb * t).astype(jnp.int32) for t in range(1, norb))
    second = pair - norb * first
    inside = pair < norb * norb
    picks = [
        jnp.where((2 * which + half == orb) & inside, 1.0, 0.0).astype(jnp.bfloat16)
        for which in (first, second)
        for half in range(2)
    ]
    picks = jnp.concatenate(picks, axis=1)
    wait()
    for i in range(norb):
        flat_ref[2 * i : 2 * i + 2, :bands] = proj_ref[0, i]
    flat = jnp.where(band_inside(flat_ref.shape, window_ref), flat_ref[...], 0.0)
    high = flat.astype(jnp.bfloat16)
    middle, low = split(flat - high.astype(jnp.float32))
    picked = lax.dot_general(
        jnp.concatenate([high, middle, low], axis=0),
        jnp.concatenate([picks, picks, picks], axis=0),
        (((0,), (0,)), ((), ())),
        preferred_element_type=jnp.float32,
    )
    i_re, i_im, j_re, j_im = (picked[:, LANES * k : LANES * (k + 1)] for k in range(4))
    pair_re = (i_re * j_re + i_im * j_im)[:bands]
    pair_im = (i_im * j_re - i_re * j_im)[:bands]
    energy = energy_ref[...]
    denom = 1.0 / (energy * energy + square)
    both = dot(-energy * denom, jnp.concatenate([pair_re, pair_im], axis=1), NN) + dot(
        freq * denom, jnp.concatenate([pair_im, -pair_re], axis=1), NN
    )
    lines = []
    for other in range(2):
        for half in range(2):
            total = both[rows * other : rows * (other + 1), LANES * half : LANES * (half + 1)]
            at = rows * (len(lines) // freqs)
            plain_ref[at : at + rows, :] = total
            lines += [total[chips * f : chips * (f + 1)] for f in range(freqs)]
    lines = pack(lines, norb)
    for r, line in enumerate(lines):
        packed_ref[pl.ds(r, chips, stride=len(lines)), :] = line


def own_sum(norb, chips, freqs, which, ref, wide_ref, mat_ref):
    pairs = norb * norb
    group = 2 * freqs
    lines = spaced(ref, chips, norb, 2 * group)[group * which : group * (which + 1)]
    mat = []
    for half in range(2):
        mat_ref[half] = upright(lines[freqs * half : freqs * (half + 1)])
        mat.append([mat_ref[half, norb * i : norb * (i + 1), :] for i in range(norb)])
    ainv = invert(*mat)
    for half in range(2):
        base = pairs * half
        for i in range(norb):
            at = base + norb * i
            ainv[half][i] = ainv[half][i] - wide_ref[at : at + norb, :]
    gorb_re, gorb_im = invert(*ainv)
    return gorb_re + gorb_im


def dress_kernel(norb, chips, freqs, own_ref, wide_ref, sum_ref, mat_ref):
    for k, row in enumerate(own_sum(norb, chips, freqs, 0, own_ref, wide_ref, mat_ref)):
        sum_ref[norb * k : norb * (k + 1), :] = row


def dyson_kernel(
    norb, chips, freqs, points, sib_ref, wide_ref, sum_ref, new_ref, tile_ref, mat_ref, turn_ref
):
    pairs = norb * norb
    group = 2 * freqs

    def rows(ref, base):
        return [ref[base + norb * i : base + norb * (i + 1), :] for i in range(norb)]

    sig_re, sig_im = rows(wide_ref, 0), rows(wide_ref, pairs)
    sums = own_sum(norb, chips, freqs, 1, sib_ref, wide_ref, mat_ref)
    sums = [a + sum_ref[norb * k : norb * (k + 1), :] for k, a in enumerate(sums)]
    shift = chips // 2
    while shift:
        sums = [a + pltpu.roll(a, LANES - shift, 1) for a in sums]
        shift //= 2
    sums = [a * (1.0 / points) for a in sums]
    inv = invert(sums[:norb], sums[norb:])
    imp = rows(wide_ref, 2 * pairs), rows(wide_ref, 3 * pairs)
    pitch = turn_ref.shape[1] // norb
    diff = [[v - m for v, m in zip(inv[half], imp[half])] for half in range(2)]
    for half in range(2):
        for i in range(norb):
            turn_ref[half, pitch * i : pitch * i + norb, :] = diff[half][i]
    mat_ref[...] = jnp.zeros_like(mat_ref)
    for half, sig, sign in ((0, sig_re, 1.0), (1, sig_im, -1.0)):
        for i in range(norb):
            across = turn_ref[half, pl.ds(i, norb, stride=pitch), :]
            fresh = sig[i] + 0.5 * (diff[half][i] + sign * across)
            mat_ref[half, norb * i : norb * (i + 1), :] = fresh
    lines = []
    for half in range(2):
        flipped = mat_ref[half].T
        lines += [flipped[chips * f : chips * f + 1] for f in range(freqs)]
    tile = jnp.concatenate(lines, axis=0)
    for half in range(2):
        for i in range(norb):
            new_ref[half, i] = tile[freqs * half : freqs * (half + 1), norb * i : norb * (i + 1)]
    lines = pack(lines, norb)
    for r, line in enumerate(lines):
        tile_ref[pl.ds(r, chips, stride=len(lines)), :] = jnp.broadcast_to(line, (chips, LANES))


def numbers_down(shape, chips, freqs, core):
    row = iota(shape, 0)
    part = row // LANES
    within = row - LANES * part
    place = within // chips
    return 2 * freqs * (within - chips * place) + freqs * (core ^ part) + place


def numbers(shape, chips, freqs, core):
    lane = iota(shape, 1)
    part = lane // LANES
    within = lane - LANES * part
    place = within // chips
    return 2 * freqs * (within - chips * place) + freqs * (core ^ part) + place


STEP = 16


def prepare_kernel(
    norb, chips, freqs, core_axis, energy_in, proj_in, window_in, sigma_ref, imp_ref, plain_ref,
    ainv_ref, green_ref, left_ref, side_ref, right_ref, wide_ref,
    energy_ref, proj_ref, window_ref, flat_ref, small_ref, sems,
):
    wait = fetched((energy_in, proj_in, window_in), (energy_ref, proj_ref, window_ref), sems)
    core = lax.axis_index(core_axis)
    pairs = norb * norb
    for which, ref in enumerate((sigma_ref, imp_ref)):
        for half in range(2):
            for i in range(norb):
                at = (which * 2 + half) * pairs + norb * i
                small_ref[at : at + norb, :] = ref[half, i]
    spread = jnp.where(iota((freqs, LANES), 1) // chips == iota((freqs, LANES), 0), 1.0, 0.0)
    wide_ref[...] = dot(small_ref[...], spread, NN)
    bands = energy_ref.shape[1]
    tall = green_ref.shape[1]
    count = green_ref.shape[2]
    rows = freqs * chips
    for part in range(2):
        mat = []
        for half in range(2):
            at = rows * (2 * part + half)
            turned = plain_ref[at : at + rows, :].T
            mat.append(rows_of(turned, norb))
        inv = invert(*mat)
        for half in range(2):
            for i in range(norb):
                ainv_ref[2 * half + part, norb * i : norb * (i + 1), :] = inv[half][i]

    flat_ref[...] = jnp.zeros_like(flat_ref)
    wait()
    for i in range(norb):
        flat_ref[i : i + 1, :bands] = proj_ref[0, i, 0:1]
        flat_ref[STEP + i : STEP + i + 1, :bands] = proj_ref[0, i, 1:2]
    flat_ref[2 * STEP : 2 * STEP + 1, :bands] = energy_ref[...]
    keep = band_inside(flat_ref.shape, window_ref) | (iota(flat_ref.shape, 0) >= 2 * STEP)
    turned = jnp.where(keep, flat_ref[...], 0.0).T[:tall]
    energy = turned[:, 2 * STEP : 2 * STEP + 1]
    freq = matsubara(numbers((tall, count), chips, freqs, core))
    denom = 1.0 / (energy * energy + freq * freq)
    green_re = -energy * denom
    green_im = -freq * denom
    green_ref[0] = green_re
    green_ref[1] = green_im
    wide = 2 * STEP
    straight = turned[:, :wide]
    high, low = split(straight)
    left_ref[...] = jnp.concatenate([high, high, low], axis=1)
    flat = jnp.where(keep, flat_ref[...], 0.0)
    span = flat.shape[1]
    energy = flat[2 * STEP : 2 * STEP + 1]
    freq = matsubara(numbers_down((count, span), chips, freqs, core))
    denom = 1.0 / (energy * energy + freq * freq)
    green_re = -energy * denom
    green_im = -freq * denom
    re, im = split(green_re), split(green_im)
    for k in range(2):
        right_ref[k, :, :span] = re[k]
        right_ref[k, :, span:] = im[k]
    side_ref[...] = jnp.zeros_like(side_ref)
    side_ref[:norb, :span] = flat[:norb]
    side_ref[:norb, span:] = flat[STEP : STEP + norb]


def solve(mat, rhs):
    size = len(mat[0])
    mat = [list(m) for m in mat]
    out = [list(r) for r in rhs]
    row = iota(mat[0][0].shape, 0)
    for p in range(size):
        at = row == p
        piv_re = mat[0][p][p : p + 1]
        piv_im = mat[1][p][p : p + 1]
        rec = 1.0 / (piv_re * piv_re + piv_im * piv_im)
        rec_re = piv_re * rec
        rec_im = -piv_im * rec
        old_re = jnp.where(at, -1.0, mat[0][p])
        old_im = jnp.where(at, 0.0, mat[1][p])
        col_re = old_re * rec_re - old_im * rec_im
        col_im = old_re * rec_im + old_im * rec_re
        for cols, start in ((mat, p + 1), (out, 0)):
            for q in range(start, size):
                x_re = cols[0][q][p : p + 1]
                x_im = cols[1][q][p : p + 1]
                rest_re = jnp.where(at, 0.0, cols[0][q])
                rest_im = jnp.where(at, 0.0, cols[1][q])
                cols[0][q] = rest_re - (col_re * x_re - col_im * x_im)
                cols[1][q] = rest_im - (col_re * x_im + col_im * x_re)
    return out


def vertex_part(norb, chips, freqs, core_axis, which, ref, ainv_ref, vert_ref, end_ref, sig_ref):
    core = lax.axis_index(core_axis)
    group = 2 * freqs
    lines = spaced(ref, chips, norb, group)
    for half in range(2):
        sig_ref[half] = upright(lines[freqs * half : freqs * (half + 1)])

    def columns(ref, first):
        return [ref[first, pl.ds(j, norb, stride=norb), :] for j in range(norb)]

    sig = [columns(sig_ref, half) for half in range(2)]
    mat = [
        [a - s for a, s in zip(columns(ainv_ref, 2 * half + which), sig[half])] for half in range(2)
    ]
    turned = solve(mat, sig)
    vert_ref[...] = jnp.zeros_like(vert_ref)
    for j in range(norb):
        sum_re, sum_im = sig[0][j], sig[1][j]
        for k in range(norb):
            y_re = turned[0][j][k : k + 1]
            y_im = turned[1][j][k : k + 1]
            sum_re = sum_re + (sig[0][k] * y_re - sig[1][k] * y_im)
            sum_im = sum_im + (sig[0][k] * y_im + sig[1][k] * y_re)
        at = 2 * LANES * j
        vert_ref[0:norb, at : at + LANES] = sum_re
        vert_ref[STEP : STEP + norb, at : at + LANES] = sum_im
        at += LANES
        vert_ref[0:norb, at : at + LANES] = sum_im
        vert_ref[STEP : STEP + norb, at : at + LANES] = -sum_re
    number = numbers((norb, 2 * LANES), chips, freqs, core)[:, LANES * which : LANES * (which + 1)]
    last = number == 2 * freqs * chips - 1
    orb = iota((norb, LANES), 1)
    end_ref[...] = jnp.zeros_like(end_ref)
    for half in range(2):
        end = jnp.zeros((norb, LANES), jnp.float32)
        for j in range(norb):
            entry = jnp.where(last, sig[half][j], 0.0)
            end = jnp.where(orb == j, jnp.sum(entry, axis=1, keepdims=True), end)
        end_ref[STEP * half : STEP * half + norb, :LANES] = end
        at = STEP * (1 - half)
        end_ref[at : at + norb, LANES:] = -end if half == 0 else end


def vertex_kernel(norb, chips, freqs, core_axis, own_ref, ainv_ref, vert_ref, end_ref, sig_ref):
    vertex_part(norb, chips, freqs, core_axis, 0, own_ref, ainv_ref, vert_ref, end_ref, sig_ref)


def density_kernel(
    norb, chips, freqs, core_axis, ainv_ref, green_ref, left_ref, side_ref, right_ref,
    first_ref, start_ref, sib_ref, out_ref, sig_ref, vert_ref, end_ref, sums_ref,
):
    bands = out_ref.shape[2]
    tall = green_ref.shape[1]
    count = green_ref.shape[2]
    vertex_part(norb, chips, freqs, core_axis, 1, sib_ref, ainv_ref, vert_ref, end_ref, sig_ref)
    left = left_ref[...]

    def mixed(block):
        high, low = split(block)
        stacked = jnp.concatenate([high, low, high], axis=0)
        return lax.dot_general(left, stacked, NN, preferred_element_type=jnp.float32)

    def doubled(halves):
        size = halves[0].shape[1] // 2
        turned = [jnp.concatenate([-h[:, size:], h[:, :size]], axis=1) for h in halves]
        return [jnp.concatenate([a, b], axis=0) for a, b in zip(halves, turned)]

    def join(re, im, right):
        left = [jnp.concatenate([r, i], axis=1) for r, i in zip(split(re), split(im))]
        return dot3(left, right, NN)

    weight = -0.5 * inverse_temp * tail_weight(count)
    tail = weight * mixed(start_ref[...] + end_ref[...])
    total = join(tail[:, :LANES], tail[:, LANES:], doubled(split(side_ref[...])))
    span = sums_ref.shape[1]
    total_re, total_im = total[:, :span], total[:, span:]
    right = doubled([right_ref[k] for k in range(2)])
    green_re, green_im = green_ref[0], green_ref[1]
    for j in range(norb):
        block = []
        for half in range(2):
            at = LANES * (2 * j + half)
            block += [first_ref[:, at : at + LANES], vert_ref[:, at : at + LANES]]
        mix = mixed(jnp.concatenate(block, axis=1))
        mix_re, mix_im = mix[:, :count], mix[:, count:]
        side_re = mix_re * green_re - mix_im * green_im
        side_im = mix_re * green_im + mix_im * green_re
        both = join(side_re, side_im, right)
        both_re, both_im = both[:, :span], both[:, span:]
        p_re = side_ref[j : j + 1, :span]
        p_im = side_ref[j : j + 1, span:]
        total_re = total_re + (both_re * p_re - both_im * p_im)
        total_im = total_im + (both_re * p_im + both_im * p_re)
    sums_ref[...] = jnp.zeros_like(sums_ref)
    for half, total, sign in ((0, total_re, 1.0), (1, total_im, -1.0)):
        sums_ref[:tall, :] = total
        both = sums_ref[...] + sign * sums_ref[...].T
        out_ref[0, half] = both[:bands, :bands] / inverse_temp


HBM = pl.BlockSpec(memory_space=pltpu.HBM)
VMEM = pl.BlockSpec(memory_space=pltpu.VMEM)


def struct(*shape, dtype=jnp.float32):
    return jax.ShapeDtypeStruct(shape, dtype)


def scratch(*shape):
    return pltpu.VMEM(shape, jnp.float32)


def run(body, out, specs, scratches=()):
    return pl.pallas_call(
        body,
        out_shape=out,
        in_specs=specs,
        out_specs=jax.tree.map(lambda _: VMEM, out),
        scratch_shapes=scratches,
        compiler_params=pltpu.CompilerParams(vmem_limit_bytes=32 * 1024 * 1024),
    )


def kernels(norb, bands, freqs, chips, cores, points):
    group = 2 * freqs
    pairs = norb * norb
    count = freqs * chips * cores
    wide = -(-bands // LANES) * LANES
    tall = -(-bands // 16) * 16
    long = kept_rows(norb, 2 * group)
    short = kept_rows(norb, group)
    axis = "core"

    def project(*refs):
        project_kernel(norb, chips, freqs, axis, *refs)

    def dyson(*refs):
        dyson_kernel(norb, chips, freqs, points, *refs)

    def prepare(*refs):
        prepare_kernel(norb, chips, freqs, axis, *refs)

    def dress(*refs):
        dress_kernel(norb, chips, freqs, *refs)

    def vertex(*refs):
        vertex_kernel(norb, chips, freqs, axis, *refs)

    def rebuild(*refs):
        density_kernel(norb, chips, freqs, axis, *refs)

    inputs = [
        pltpu.VMEM((1, bands), jnp.float32),
        pltpu.VMEM((1, norb, 2, bands), jnp.float32),
        pltpu.VMEM((1, 2), jnp.int32),
    ]
    first = run(
        project,
        (struct(chips * long, LANES), struct(2 * count, LANES)),
        [HBM] * 3,
        [*inputs, scratch(32, wide), pltpu.SemaphoreType.DMA((3,))],
    )
    second = run(
        dyson,
        (struct(2, norb, freqs, norb), struct(chips * short, LANES)),
        [VMEM] * 3,
        [scratch(2, LANES, LANES), scratch(2, 16 * norb, LANES)],
    )
    before = run(dress, struct(2 * pairs, LANES), [VMEM] * 2, [scratch(2, LANES, LANES)])
    after = run(
        vertex,
        (struct(2 * STEP, 2 * norb * LANES), struct(2 * STEP, 2 * LANES)),
        [VMEM] * 2,
        [scratch(2, LANES, LANES)],
    )
    aside = run(
        prepare,
        (
            struct(4, pairs, LANES),
            struct(2, tall, count),
            struct(tall, 6 * STEP, dtype=jnp.bfloat16),
            struct(LANES, 2 * wide),
            struct(2, count, 2 * wide, dtype=jnp.bfloat16),
            struct(4 * pairs, LANES),
        ),
        [HBM] * 3 + [VMEM] * 3,
        [
            *inputs,
            scratch(LANES, wide),
            scratch(4 * pairs, freqs),
            pltpu.SemaphoreType.DMA((3,)),
        ],
    )
    third = run(
        rebuild,
        struct(1, 2, bands, bands),
        [VMEM] * 8,
        [
            scratch(2, LANES, LANES),
            scratch(2 * STEP, 2 * norb * LANES),
            scratch(2 * STEP, 2 * LANES),
            scratch(wide, wide),
        ],
    )
    return first, aside, before, second, after, third


def local(energies, proj, window, sigma, impurity_inverse):
    norb, bands = proj.shape[2:]
    freqs = sigma.shape[3]
    chips = lax.axis_size("z")
    cores = lax.axis_size("core")
    points = energies.shape[0] * chips * cores
    first, aside, before, second, after, third = kernels(norb, bands, freqs, chips, cores, points)
    swap = [(0, 1), (1, 0)]
    proj = jnp.swapaxes(proj, 1, 2)

    def across(rows):
        got = lax.all_to_all(rows.reshape(chips, 1, -1), "z", 0, 0, tiled=True)
        return got.reshape(rows.shape)

    far = [pltpu.with_memory_space_constraint(x, pltpu.HBM) for x in (energies, proj, window)]
    packed, plain = first(*far)
    ready = aside(*far, sigma, impurity_inverse, plain)
    got, ready = lax.optimization_barrier((across(packed), ready))
    *ready, spread = ready
    sibling = lax.ppermute(got, "core", swap)
    sigma_new, tiles = second(sibling, spread, before(got, spread))
    back = across(tiles)
    sibling = lax.ppermute(back, "core", swap)
    density = third(*ready, *after(back, ready[0]), sibling)
    return density, jnp.swapaxes(sigma_new, 2, 3)


def solution(mesh):
    parts, line = mesh.shape["parts"], mesh.shape["ka"]
    torus = Mesh(mesh.devices.reshape(parts, line // 2, 2), ("parts", "z", "core"))
    every = ("parts", "z", "core")
    line = ("z", "core")
    in_specs = (
        P(every, None),
        P(every, None, None, None),
        P(every, None),
        P("parts", None, None, line),
        P("parts", None, None, line),
    )
    out_specs = (P(every, None, None, None), P("parts", None, None, line))
    return jax.shard_map(local, mesh=torus, in_specs=in_specs, out_specs=out_specs, check_vma=False)
```

```python
import math

import jax
import jax.numpy as jnp
from jax import lax
from jax.experimental import pallas as pl
from jax.experimental.pallas import tpu as pltpu
from jax.sharding import Mesh
from jax.sharding import PartitionSpec as P

highest = lax.Precision.HIGHEST
inverse_temp = 40.0
LANES = 128
NN = (((1,), (0,)), ((), ()))
NT = (((1,), (1,)), ((), ()))


def tail_weight(count):
    total = 0.0
    for number in range(count):
        total += (inverse_temp / (math.pi * (2 * number + 1))) ** 2
    return inverse_temp / 4.0 - 2.0 / inverse_temp * total


def dot(a, b, dims, precision=highest):
    return lax.dot_general(a, b, dims, precision=precision, preferred_element_type=jnp.float32)


def split(x):
    high = x.astype(jnp.bfloat16)
    return high, (x - high.astype(jnp.float32)).astype(jnp.bfloat16)


def dot3(a, b, dims):
    return sum(
        lax.dot_general(x, y, dims, preferred_element_type=jnp.float32)
        for x, y in ((a[0], b[0]), (a[0], b[1]), (a[1], b[0]))
    )


def iota(shape, dim):
    return lax.broadcasted_iota(jnp.int32, shape, dim)


def matsubara(number):
    return (2.0 * number.astype(jnp.float32) + 1.0) * (math.pi / inverse_temp)


def spare_of(norb):
    used = norb * norb
    width = LANES - used
    pieces = -(-used // width)
    return used, width, pieces


def kept_rows(norb, rows):
    pieces = spare_of(norb)[2]
    extra = 0
    while pieces * (extra + 1) <= rows - (extra + 1):
        extra += 1
    return rows - extra


def pack(rows, norb):
    used, width, pieces = spare_of(norb)
    kept = kept_rows(norb, len(rows))
    out = list(rows[:kept])
    lane = iota(rows[0].shape, 1)
    for e, row in enumerate(rows[kept:]):
        for p in range(pieces):
            moved = pltpu.roll(row, (used - width * p) % LANES, 1)
            out[pieces * e + p] = jnp.where(lane < used, out[pieces * e + p], moved)
    return out


def unpack(kept, norb, rows):
    used, width, pieces = spare_of(norb)
    out = list(kept)
    lane = iota(kept[0].shape, 1)
    for e in range(rows - len(kept)):
        row = 0.0
        for p in range(pieces):
            moved = pltpu.roll(kept[pieces * e + p], (width * p - used) % LANES, 1)
            inside = (lane >= width * p) & (lane < min(width * (p + 1), used))
            row = jnp.where(inside, moved, row)
        out.append(row)
    return out


def spaced(ref, chips, norb, rows):
    pitch = kept_rows(norb, rows)
    return unpack([ref[pl.ds(r, chips, stride=pitch), :] for r in range(pitch)], norb, rows)


def upright(rows):
    return jnp.concatenate(rows, axis=0).T


def invert(mat_re, mat_im):
    size = len(mat_re)
    mat_re, mat_im = list(mat_re), list(mat_im)
    column = iota(mat_re[0].shape, 0)
    for p in range(size):
        at = column == p
        piv_re = mat_re[p][p : p + 1]
        piv_im = mat_im[p][p : p + 1]
        rec = 1.0 / (piv_re * piv_re + piv_im * piv_im)
        rec_re = piv_re * rec
        rec_im = -piv_im * rec
        old_re = jnp.where(at, 1.0, mat_re[p])
        old_im = jnp.where(at, 0.0, mat_im[p])
        row_re = old_re * rec_re - old_im * rec_im
        row_im = old_re * rec_im + old_im * rec_re
        for i in range(size):
            if i == p:
                continue
            col_re = mat_re[i][p : p + 1]
            col_im = mat_im[i][p : p + 1]
            rest_re = jnp.where(at, 0.0, mat_re[i])
            rest_im = jnp.where(at, 0.0, mat_im[i])
            mat_re[i] = rest_re - (col_re * row_re - col_im * row_im)
            mat_im[i] = rest_im - (col_re * row_im + col_im * row_re)
        mat_re[p] = row_re
        mat_im[p] = row_im
    return mat_re, mat_im


def rows_of(block, norb):
    return [block[norb * i : norb * (i + 1)] for i in range(norb)]


def fetched(sources, targets, sems):
    copies = [pltpu.make_async_copy(a, b, sems.at[k]) for k, (a, b) in enumerate(zip(sources, targets))]
    for copy in copies:
        copy.start()

    def wait():
        for copy in copies:
            copy.wait()

    return wait


def band_inside(shape, window_ref):
    band = iota(shape, 1)
    return (band >= window_ref[:, 0:1]) & (band < window_ref[:, 1:2])


def project_kernel(
    norb, chips, freqs, core_axis, energy_in, proj_in, window_in, packed_ref, plain_ref,
    energy_ref, proj_ref, window_ref, flat_ref, sems,
):
    wait = fetched((energy_in, proj_in, window_in), (energy_ref, proj_ref, window_ref), sems)
    core = lax.axis_index(core_axis)
    bands = energy_ref.shape[1]
    rows = freqs * chips
    flat_ref[...] = jnp.zeros_like(flat_ref)
    freq = matsubara(numbers_down((2 * rows, bands), chips, freqs, core))
    square = freq * freq
    pair = iota((flat_ref.shape[0], LANES), 1)
    orb = iota((flat_ref.shape[0], LANES), 0)
    first = sum((pair >= norb * t).astype(jnp.int32) for t in range(1, norb))
    second = pair - norb * first
    inside = pair < norb * norb
    picks = [
        jnp.where((2 * which + half == orb) & inside, 1.0, 0.0).astype(jnp.bfloat16)
        for which in (first, second)
        for half in range(2)
    ]
    picks = jnp.concatenate(picks, axis=1)
    wait()
    for i in range(norb):
        flat_ref[2 * i : 2 * i + 2, :bands] = proj_ref[0, i]
    flat = jnp.where(band_inside(flat_ref.shape, window_ref), flat_ref[...], 0.0)
    high = flat.astype(jnp.bfloat16)
    middle, low = split(flat - high.astype(jnp.float32))
    picked = lax.dot_general(
        jnp.concatenate([high, middle, low], axis=0),
        jnp.concatenate([picks, picks, picks], axis=0),
        (((0,), (0,)), ((), ())),
        preferred_element_type=jnp.float32,
    )
    i_re, i_im, j_re, j_im = (picked[:, LANES * k : LANES * (k + 1)] for k in range(4))
    pair_re = (i_re * j_re + i_im * j_im)[:bands]
    pair_im = (i_im * j_re - i_re * j_im)[:bands]
    energy = energy_ref[...]
    denom = 1.0 / (energy * energy + square)
    both = dot(-energy * denom, jnp.concatenate([pair_re, pair_im], axis=1), NN) + dot(
        freq * denom, jnp.concatenate([pair_im, -pair_re], axis=1), NN
    )
    lines = []
    for other in range(2):
        for half in range(2):
            total = both[rows * other : rows * (other + 1), LANES * half : LANES * (half + 1)]
            at = rows * (len(lines) // freqs)
            plain_ref[at : at + rows, :] = total
            lines += [total[chips * f : chips * (f + 1)] for f in range(freqs)]
    lines = pack(lines, norb)
    for r, line in enumerate(lines):
        packed_ref[pl.ds(r, chips, stride=len(lines)), :] = line


def own_sum(norb, chips, freqs, which, ref, wide_ref, mat_ref):
    pairs = norb * norb
    group = 2 * freqs
    lines = spaced(ref, chips, norb, 2 * group)[group * which : group * (which + 1)]
    mat = []
    for half in range(2):
        mat_ref[half] = upright(lines[freqs * half : freqs * (half + 1)])
        mat.append([mat_ref[half, norb * i : norb * (i + 1), :] for i in range(norb)])
    ainv = invert(*mat)
    for half in range(2):
        base = pairs * half
        for i in range(norb):
            at = base + norb * i
            ainv[half][i] = ainv[half][i] - wide_ref[at : at + norb, :]
    gorb_re, gorb_im = invert(*ainv)
    return gorb_re + gorb_im


def dress_kernel(norb, chips, freqs, own_ref, wide_ref, sum_ref, mat_ref):
    for k, row in enumerate(own_sum(norb, chips, freqs, 0, own_ref, wide_ref, mat_ref)):
        sum_ref[norb * k : norb * (k + 1), :] = row


def dyson_kernel(
    norb, chips, freqs, points, sib_ref, wide_ref, sum_ref, new_ref, tile_ref, mat_ref, turn_ref
):
    pairs = norb * norb
    group = 2 * freqs

    def rows(ref, base):
        return [ref[base + norb * i : base + norb * (i + 1), :] for i in range(norb)]

    sig_re, sig_im = rows(wide_ref, 0), rows(wide_ref, pairs)
    sums = own_sum(norb, chips, freqs, 1, sib_ref, wide_ref, mat_ref)
    sums = [a + sum_ref[norb * k : norb * (k + 1), :] for k, a in enumerate(sums)]
    shift = chips // 2
    while shift:
        sums = [a + pltpu.roll(a, LANES - shift, 1) for a in sums]
        shift //= 2
    sums = [a * (1.0 / points) for a in sums]
    inv = invert(sums[:norb], sums[norb:])
    imp = rows(wide_ref, 2 * pairs), rows(wide_ref, 3 * pairs)
    pitch = turn_ref.shape[1] // norb
    diff = [[v - m for v, m in zip(inv[half], imp[half])] for half in range(2)]
    for half in range(2):
        for i in range(norb):
            turn_ref[half, pitch * i : pitch * i + norb, :] = diff[half][i]
    mat_ref[...] = jnp.zeros_like(mat_ref)
    for half, sig, sign in ((0, sig_re, 1.0), (1, sig_im, -1.0)):
        for i in range(norb):
            across = turn_ref[half, pl.ds(i, norb, stride=pitch), :]
            fresh = sig[i] + 0.5 * (diff[half][i] + sign * across)
            mat_ref[half, norb * i : norb * (i + 1), :] = fresh
    lines = []
    for half in range(2):
        flipped = mat_ref[half].T
        lines += [flipped[chips * f : chips * f + 1] for f in range(freqs)]
    tile = jnp.concatenate(lines, axis=0)
    for half in range(2):
        for i in range(norb):
            new_ref[half, i] = tile[freqs * half : freqs * (half + 1), norb * i : norb * (i + 1)]
    lines = pack(lines, norb)
    for r, line in enumerate(lines):
        tile_ref[pl.ds(r, chips, stride=len(lines)), :] = jnp.broadcast_to(line, (chips, LANES))


def numbers_down(shape, chips, freqs, core):
    row = iota(shape, 0)
    part = row // LANES
    within = row - LANES * part
    place = within // chips
    return 2 * freqs * (within - chips * place) + freqs * (core ^ part) + place


def numbers(shape, chips, freqs, core):
    lane = iota(shape, 1)
    part = lane // LANES
    within = lane - LANES * part
    place = within // chips
    return 2 * freqs * (within - chips * place) + freqs * (core ^ part) + place


STEP = 16


def prepare_kernel(
    norb, chips, freqs, core_axis, energy_in, proj_in, window_in, sigma_ref, imp_ref, plain_ref,
    ainv_ref, green_ref, left_ref, side_ref, right_ref, wide_ref,
    energy_ref, proj_ref, window_ref, flat_ref, small_ref, sems,
):
    wait = fetched((energy_in, proj_in, window_in), (energy_ref, proj_ref, window_ref), sems)
    core = lax.axis_index(core_axis)
    pairs = norb * norb
    for which, ref in enumerate((sigma_ref, imp_ref)):
        for half in range(2):
            for i in range(norb):
                at = (which * 2 + half) * pairs + norb * i
                small_ref[at : at + norb, :] = ref[half, i]
    spread = jnp.where(iota((freqs, LANES), 1) // chips == iota((freqs, LANES), 0), 1.0, 0.0)
    wide_ref[...] = dot(small_ref[...], spread, NN)
    bands = energy_ref.shape[1]
    tall = green_ref.shape[1]
    count = green_ref.shape[2]
    rows = freqs * chips
    for part in range(2):
        mat = []
        for half in range(2):
            at = rows * (2 * part + half)
            turned = plain_ref[at : at + rows, :].T
            mat.append(rows_of(turned, norb))
        inv = invert(*mat)
        for half in range(2):
            for i in range(norb):
                ainv_ref[2 * half + part, norb * i : norb * (i + 1), :] = inv[half][i]

    flat_ref[...] = jnp.zeros_like(flat_ref)
    wait()
    for i in range(norb):
        flat_ref[i : i + 1, :bands] = proj_ref[0, i, 0:1]
        flat_ref[STEP + i : STEP + i + 1, :bands] = proj_ref[0, i, 1:2]
    flat_ref[2 * STEP : 2 * STEP + 1, :bands] = energy_ref[...]
    keep = band_inside(flat_ref.shape, window_ref) | (iota(flat_ref.shape, 0) >= 2 * STEP)
    turned = jnp.where(keep, flat_ref[...], 0.0).T[:tall]
    energy = turned[:, 2 * STEP : 2 * STEP + 1]
    freq = matsubara(numbers((tall, count), chips, freqs, core))
    denom = 1.0 / (energy * energy + freq * freq)
    green_re = -energy * denom
    green_im = -freq * denom
    green_ref[0] = green_re
    green_ref[1] = green_im
    wide = 2 * STEP
    straight = turned[:, :wide]
    high, low = split(straight)
    left_ref[...] = jnp.concatenate([high, high, low], axis=1)
    flat = jnp.where(keep, flat_ref[...], 0.0)
    span = flat.shape[1]
    energy = flat[2 * STEP : 2 * STEP + 1]
    freq = matsubara(numbers_down((count, span), chips, freqs, core))
    denom = 1.0 / (energy * energy + freq * freq)
    green_re = -energy * denom
    green_im = -freq * denom
    re, im = split(green_re), split(green_im)
    for k in range(2):
        right_ref[k, :, :span] = re[k]
        right_ref[k, :, span:] = im[k]
    side_ref[...] = jnp.zeros_like(side_ref)
    side_ref[:norb, :span] = flat[:norb]
    side_ref[:norb, span:] = flat[STEP : STEP + norb]


def solve(mat, rhs):
    size = len(mat[0])
    mat = [list(m) for m in mat]
    out = [list(r) for r in rhs]
    row = iota(mat[0][0].shape, 0)
    for p in range(size):
        at = row == p
        piv_re = mat[0][p][p : p + 1]
        piv_im = mat[1][p][p : p + 1]
        rec = 1.0 / (piv_re * piv_re + piv_im * piv_im)
        rec_re = piv_re * rec
        rec_im = -piv_im * rec
        old_re = jnp.where(at, -1.0, mat[0][p])
        old_im = jnp.where(at, 0.0, mat[1][p])
        col_re = old_re * rec_re - old_im * rec_im
        col_im = old_re * rec_im + old_im * rec_re
        for cols, start in ((mat, p + 1), (out, 0)):
            for q in range(start, size):
                x_re = cols[0][q][p : p + 1]
                x_im = cols[1][q][p : p + 1]
                rest_re = jnp.where(at, 0.0, cols[0][q])
                rest_im = jnp.where(at, 0.0, cols[1][q])
                cols[0][q] = rest_re - (col_re * x_re - col_im * x_im)
                cols[1][q] = rest_im - (col_re * x_im + col_im * x_re)
    return out


def vertex_part(norb, chips, freqs, core_axis, which, ref, ainv_ref, vert_ref, end_ref, sig_ref):
    core = lax.axis_index(core_axis)
    group = 2 * freqs
    lines = spaced(ref, chips, norb, group)
    for half in range(2):
        sig_ref[half] = upright(lines[freqs * half : freqs * (half + 1)])

    def columns(ref, first):
        return [ref[first, pl.ds(j, norb, stride=norb), :] for j in range(norb)]

    sig = [columns(sig_ref, half) for half in range(2)]
    mat = [
        [a - s for a, s in zip(columns(ainv_ref, 2 * half + which), sig[half])] for half in range(2)
    ]
    turned = solve(mat, sig)
    vert_ref[...] = jnp.zeros_like(vert_ref)
    for j in range(norb):
        sum_re, sum_im = sig[0][j], sig[1][j]
        for k in range(norb):
            y_re = turned[0][j][k : k + 1]
            y_im = turned[1][j][k : k + 1]
            sum_re = sum_re + (sig[0][k] * y_re - sig[1][k] * y_im)
            sum_im = sum_im + (sig[0][k] * y_im + sig[1][k] * y_re)
        at = 2 * LANES * j
        vert_ref[0:norb, at : at + LANES] = sum_re
        vert_ref[STEP : STEP + norb, at : at + LANES] = sum_im
        at += LANES
        vert_ref[0:norb, at : at + LANES] = sum_im
        vert_ref[STEP : STEP + norb, at : at + LANES] = -sum_re
    number = numbers((norb, 2 * LANES), chips, freqs, core)[:, LANES * which : LANES * (which + 1)]
    last = number == 2 * freqs * chips - 1
    orb = iota((norb, LANES), 1)
    end_ref[...] = jnp.zeros_like(end_ref)
    for half in range(2):
        end = jnp.zeros((norb, LANES), jnp.float32)
        for j in range(norb):
            entry = jnp.where(last, sig[half][j], 0.0)
            end = jnp.where(orb == j, jnp.sum(entry, axis=1, keepdims=True), end)
        end_ref[STEP * half : STEP * half + norb, :LANES] = end
        at = STEP * (1 - half)
        end_ref[at : at + norb, LANES:] = -end if half == 0 else end


def vertex_kernel(norb, chips, freqs, core_axis, own_ref, ainv_ref, vert_ref, end_ref, sig_ref):
    vertex_part(norb, chips, freqs, core_axis, 0, own_ref, ainv_ref, vert_ref, end_ref, sig_ref)


def density_kernel(
    norb, chips, freqs, core_axis, ainv_ref, green_ref, left_ref, side_ref, right_ref,
    first_ref, start_ref, sib_ref, out_ref, sig_ref, vert_ref, end_ref, sums_ref,
):
    bands = out_ref.shape[2]
    tall = green_ref.shape[1]
    count = green_ref.shape[2]
    vertex_part(norb, chips, freqs, core_axis, 1, sib_ref, ainv_ref, vert_ref, end_ref, sig_ref)
    left = left_ref[...]

    def mixed(block):
        high, low = split(block)
        stacked = jnp.concatenate([high, low, high], axis=0)
        return lax.dot_general(left, stacked, NN, preferred_element_type=jnp.float32)

    def doubled(halves):
        size = halves[0].shape[1] // 2
        turned = [jnp.concatenate([-h[:, size:], h[:, :size]], axis=1) for h in halves]
        return [jnp.concatenate([a, b], axis=0) for a, b in zip(halves, turned)]

    def join(re, im, right):
        left = [jnp.concatenate([r, i], axis=1) for r, i in zip(split(re), split(im))]
        return dot3(left, right, NN)

    weight = -0.5 * inverse_temp * tail_weight(count)
    tail = weight * mixed(start_ref[...] + end_ref[...])
    total = join(tail[:, :LANES], tail[:, LANES:], doubled(split(side_ref[...])))
    span = sums_ref.shape[1]
    total_re, total_im = total[:, :span], total[:, span:]
    right_re = [right_ref[k, :, :span] for k in range(2)]
    right_im = [right_ref[k, :, span:] for k in range(2)]
    right_sum = split(
        (right_re[0].astype(jnp.float32) + right_im[0].astype(jnp.float32))
        + (right_re[1].astype(jnp.float32) + right_im[1].astype(jnp.float32))
    )
    green_re, green_im = green_ref[0], green_ref[1]
    for j in range(norb):
        block = []
        for half in range(2):
            at = LANES * (2 * j + half)
            block += [first_ref[:, at : at + LANES], vert_ref[:, at : at + LANES]]
        mix = mixed(jnp.concatenate(block, axis=1))
        mix_re, mix_im = mix[:, :count], mix[:, count:]
        side_re = mix_re * green_re - mix_im * green_im
        side_im = mix_re * green_im + mix_im * green_re
        prod_re = dot3(split(side_re), right_re, NN)
        prod_im = dot3(split(side_im), right_im, NN)
        prod_sum = dot3(split(side_re + side_im), right_sum, NN)
        both_re = prod_re - prod_im
        both_im = prod_sum - prod_re - prod_im
        p_re = side_ref[j : j + 1, :span]
        p_im = side_ref[j : j + 1, span:]
        total_re = total_re + (both_re * p_re - both_im * p_im)
        total_im = total_im + (both_re * p_im + both_im * p_re)
    sums_ref[...] = jnp.zeros_like(sums_ref)
    for half, total, sign in ((0, total_re, 1.0), (1, total_im, -1.0)):
        sums_ref[:tall, :] = total
        both = sums_ref[...] + sign * sums_ref[...].T
        out_ref[0, half] = both[:bands, :bands] / inverse_temp


HBM = pl.BlockSpec(memory_space=pltpu.HBM)
VMEM = pl.BlockSpec(memory_space=pltpu.VMEM)


def struct(*shape, dtype=jnp.float32):
    return jax.ShapeDtypeStruct(shape, dtype)


def scratch(*shape):
    return pltpu.VMEM(shape, jnp.float32)


def run(body, out, specs, scratches=()):
    return pl.pallas_call(
        body,
        out_shape=out,
        in_specs=specs,
        out_specs=jax.tree.map(lambda _: VMEM, out),
        scratch_shapes=scratches,
        compiler_params=pltpu.CompilerParams(vmem_limit_bytes=32 * 1024 * 1024),
    )


def kernels(norb, bands, freqs, chips, cores, points):
    group = 2 * freqs
    pairs = norb * norb
    count = freqs * chips * cores
    wide = -(-bands // LANES) * LANES
    tall = -(-bands // 16) * 16
    long = kept_rows(norb, 2 * group)
    short = kept_rows(norb, group)
    axis = "core"

    def project(*refs):
        project_kernel(norb, chips, freqs, axis, *refs)

    def dyson(*refs):
        dyson_kernel(norb, chips, freqs, points, *refs)

    def prepare(*refs):
        prepare_kernel(norb, chips, freqs, axis, *refs)

    def dress(*refs):
        dress_kernel(norb, chips, freqs, *refs)

    def vertex(*refs):
        vertex_kernel(norb, chips, freqs, axis, *refs)

    def rebuild(*refs):
        density_kernel(norb, chips, freqs, axis, *refs)

    inputs = [
        pltpu.VMEM((1, bands), jnp.float32),
        pltpu.VMEM((1, norb, 2, bands), jnp.float32),
        pltpu.VMEM((1, 2), jnp.int32),
    ]
    first = run(
        project,
        (struct(chips * long, LANES), struct(2 * count, LANES)),
        [HBM] * 3,
        [*inputs, scratch(32, wide), pltpu.SemaphoreType.DMA((3,))],
    )
    second = run(
        dyson,
        (struct(2, norb, freqs, norb), struct(chips * short, LANES)),
        [VMEM] * 3,
        [scratch(2, LANES, LANES), scratch(2, 16 * norb, LANES)],
    )
    before = run(dress, struct(2 * pairs, LANES), [VMEM] * 2, [scratch(2, LANES, LANES)])
    after = run(
        vertex,
        (struct(2 * STEP, 2 * norb * LANES), struct(2 * STEP, 2 * LANES)),
        [VMEM] * 2,
        [scratch(2, LANES, LANES)],
    )
    aside = run(
        prepare,
        (
            struct(4, pairs, LANES),
            struct(2, tall, count),
            struct(tall, 6 * STEP, dtype=jnp.bfloat16),
            struct(LANES, 2 * wide),
            struct(2, count, 2 * wide, dtype=jnp.bfloat16),
            struct(4 * pairs, LANES),
        ),
        [HBM] * 3 + [VMEM] * 3,
        [
            *inputs,
            scratch(LANES, wide),
            scratch(4 * pairs, freqs),
            pltpu.SemaphoreType.DMA((3,)),
        ],
    )
    third = run(
        rebuild,
        struct(1, 2, bands, bands),
        [VMEM] * 8,
        [
            scratch(2, LANES, LANES),
            scratch(2 * STEP, 2 * norb * LANES),
            scratch(2 * STEP, 2 * LANES),
            scratch(wide, wide),
        ],
    )
    return first, aside, before, second, after, third


def local(energies, proj, window, sigma, impurity_inverse):
    norb, bands = proj.shape[2:]
    freqs = sigma.shape[3]
    chips = lax.axis_size("z")
    cores = lax.axis_size("core")
    points = energies.shape[0] * chips * cores
    first, aside, before, second, after, third = kernels(norb, bands, freqs, chips, cores, points)
    swap = [(0, 1), (1, 0)]
    proj = jnp.swapaxes(proj, 1, 2)

    def across(rows):
        got = lax.all_to_all(rows.reshape(chips, 1, -1), "z", 0, 0, tiled=True)
        return got.reshape(rows.shape)

    far = [pltpu.with_memory_space_constraint(x, pltpu.HBM) for x in (energies, proj, window)]
    packed, plain = first(*far)
    ready = aside(*far, sigma, impurity_inverse, plain)
    got, ready = lax.optimization_barrier((across(packed), ready))
    *ready, spread = ready
    sibling = lax.ppermute(got, "core", swap)
    sigma_new, tiles = second(sibling, spread, before(got, spread))
    back = across(tiles)
    sibling = lax.ppermute(back, "core", swap)
    density = third(*ready, *after(back, ready[0]), sibling)
    return density, jnp.swapaxes(sigma_new, 2, 3)


def solution(mesh):
    parts, line = mesh.shape["parts"], mesh.shape["ka"]
    torus = Mesh(mesh.devices.reshape(parts, line // 2, 2), ("parts", "z", "core"))
    every = ("parts", "z", "core")
    line = ("z", "core")
    in_specs = (
        P(every, None),
        P(every, None, None, None),
        P(every, None),
        P("parts", None, None, line),
        P("parts", None, None, line),
    )
    out_specs = (P(every, None, None, None), P("parts", None, None, line))
    return jax.shard_map(local, mesh=torus, in_specs=in_specs, out_specs=out_specs, check_vma=False)
```

```python
import math

import jax
import jax.numpy as jnp
from jax import lax
from jax.experimental import pallas as pl
from jax.experimental.pallas import tpu as pltpu
from jax.sharding import Mesh
from jax.sharding import PartitionSpec as P

highest = lax.Precision.HIGHEST
inverse_temp = 40.0
LANES = 128
NN = (((1,), (0,)), ((), ()))
NT = (((1,), (1,)), ((), ()))


def tail_weight(count):
    total = 0.0
    for number in range(count):
        total += (inverse_temp / (math.pi * (2 * number + 1))) ** 2
    return inverse_temp / 4.0 - 2.0 / inverse_temp * total


def dot(a, b, dims, precision=highest):
    return lax.dot_general(a, b, dims, precision=precision, preferred_element_type=jnp.float32)


def split(x):
    high = x.astype(jnp.bfloat16)
    return high, (x - high.astype(jnp.float32)).astype(jnp.bfloat16)


def dot3(a, b, dims):
    return sum(
        lax.dot_general(x, y, dims, preferred_element_type=jnp.float32)
        for x, y in ((a[0], b[0]), (a[0], b[1]), (a[1], b[0]))
    )


def iota(shape, dim):
    return lax.broadcasted_iota(jnp.int32, shape, dim)


def matsubara(number):
    return (2.0 * number.astype(jnp.float32) + 1.0) * (math.pi / inverse_temp)


def spare_of(norb):
    used = norb * norb
    width = LANES - used
    pieces = -(-used // width)
    return used, width, pieces


def kept_rows(norb, rows):
    pieces = spare_of(norb)[2]
    extra = 0
    while pieces * (extra + 1) <= rows - (extra + 1):
        extra += 1
    return rows - extra


def pack(rows, norb):
    used, width, pieces = spare_of(norb)
    kept = kept_rows(norb, len(rows))
    out = list(rows[:kept])
    lane = iota(rows[0].shape, 1)
    for e, row in enumerate(rows[kept:]):
        for p in range(pieces):
            moved = pltpu.roll(row, (used - width * p) % LANES, 1)
            out[pieces * e + p] = jnp.where(lane < used, out[pieces * e + p], moved)
    return out


def unpack(kept, norb, rows):
    used, width, pieces = spare_of(norb)
    out = list(kept)
    lane = iota(kept[0].shape, 1)
    for e in range(rows - len(kept)):
        row = 0.0
        for p in range(pieces):
            moved = pltpu.roll(kept[pieces * e + p], (width * p - used) % LANES, 1)
            inside = (lane >= width * p) & (lane < min(width * (p + 1), used))
            row = jnp.where(inside, moved, row)
        out.append(row)
    return out


def spaced(ref, chips, norb, rows):
    pitch = kept_rows(norb, rows)
    return unpack([ref[pl.ds(r, chips, stride=pitch), :] for r in range(pitch)], norb, rows)


def upright(rows):
    return jnp.concatenate(rows, axis=0).T


def invert(mat_re, mat_im):
    size = len(mat_re)
    mat_re, mat_im = list(mat_re), list(mat_im)
    column = iota(mat_re[0].shape, 0)
    for p in range(size):
        at = column == p
        piv_re = mat_re[p][p : p + 1]
        piv_im = mat_im[p][p : p + 1]
        rec = 1.0 / (piv_re * piv_re + piv_im * piv_im)
        rec_re = piv_re * rec
        rec_im = -piv_im * rec
        old_re = jnp.where(at, 1.0, mat_re[p])
        old_im = jnp.where(at, 0.0, mat_im[p])
        row_re = old_re * rec_re - old_im * rec_im
        row_im = old_re * rec_im + old_im * rec_re
        for i in range(size):
            if i == p:
                continue
            col_re = mat_re[i][p : p + 1]
            col_im = mat_im[i][p : p + 1]
            rest_re = jnp.where(at, 0.0, mat_re[i])
            rest_im = jnp.where(at, 0.0, mat_im[i])
            mat_re[i] = rest_re - (col_re * row_re - col_im * row_im)
            mat_im[i] = rest_im - (col_re * row_im + col_im * row_re)
        mat_re[p] = row_re
        mat_im[p] = row_im
    return mat_re, mat_im


def rows_of(block, norb):
    return [block[norb * i : norb * (i + 1)] for i in range(norb)]


def fetched(sources, targets, sems):
    copies = [pltpu.make_async_copy(a, b, sems.at[k]) for k, (a, b) in enumerate(zip(sources, targets))]
    for copy in copies:
        copy.start()

    def wait():
        for copy in copies:
            copy.wait()

    return wait


def band_inside(shape, window_ref):
    band = iota(shape, 1)
    return (band >= window_ref[:, 0:1]) & (band < window_ref[:, 1:2])


def project_kernel(
    norb, chips, freqs, core_axis, energy_in, proj_in, window_in, packed_ref, plain_ref,
    energy_ref, proj_ref, window_ref, flat_ref, sems,
):
    wait = fetched((energy_in, proj_in, window_in), (energy_ref, proj_ref, window_ref), sems)
    core = lax.axis_index(core_axis)
    bands = energy_ref.shape[1]
    rows = freqs * chips
    flat_ref[...] = jnp.zeros_like(flat_ref)
    freq = matsubara(numbers_down((2 * rows, bands), chips, freqs, core))
    square = freq * freq
    pair = iota((flat_ref.shape[0], LANES), 1)
    orb = iota((flat_ref.shape[0], LANES), 0)
    first = sum((pair >= norb * t).astype(jnp.int32) for t in range(1, norb))
    second = pair - norb * first
    inside = pair < norb * norb
    picks = [
        jnp.where((2 * which + half == orb) & inside, 1.0, 0.0).astype(jnp.bfloat16)
        for which in (first, second)
        for half in range(2)
    ]
    picks = jnp.concatenate(picks, axis=1)
    wait()
    for i in range(norb):
        flat_ref[2 * i : 2 * i + 2, :bands] = proj_ref[0, i]
    flat = jnp.where(band_inside(flat_ref.shape, window_ref), flat_ref[...], 0.0)
    high = flat.astype(jnp.bfloat16)
    middle, low = split(flat - high.astype(jnp.float32))
    picked = lax.dot_general(
        jnp.concatenate([high, middle, low], axis=0),
        jnp.concatenate([picks, picks, picks], axis=0),
        (((0,), (0,)), ((), ())),
        preferred_element_type=jnp.float32,
    )
    i_re, i_im, j_re, j_im = (picked[:, LANES * k : LANES * (k + 1)] for k in range(4))
    pair_re = (i_re * j_re + i_im * j_im)[:bands]
    pair_im = (i_im * j_re - i_re * j_im)[:bands]
    energy = energy_ref[...]
    denom = 1.0 / (energy * energy + square)
    both = dot(-energy * denom, jnp.concatenate([pair_re, pair_im], axis=1), NN) + dot(
        freq * denom, jnp.concatenate([pair_im, -pair_re], axis=1), NN
    )
    lines = []
    for other in range(2):
        for half in range(2):
            total = both[rows * other : rows * (other + 1), LANES * half : LANES * (half + 1)]
            at = rows * (len(lines) // freqs)
            plain_ref[at : at + rows, :] = total
            lines += [total[chips * f : chips * (f + 1)] for f in range(freqs)]
    lines = pack(lines, norb)
    for r, line in enumerate(lines):
        packed_ref[pl.ds(r, chips, stride=len(lines)), :] = line


def own_sum(norb, chips, freqs, which, ref, wide_ref, mat_ref):
    pairs = norb * norb
    group = 2 * freqs
    lines = spaced(ref, chips, norb, 2 * group)[group * which : group * (which + 1)]
    mat = []
    for half in range(2):
        mat_ref[half] = upright(lines[freqs * half : freqs * (half + 1)])
        mat.append([mat_ref[half, norb * i : norb * (i + 1), :] for i in range(norb)])
    ainv = invert(*mat)
    for half in range(2):
        base = pairs * half
        for i in range(norb):
            at = base + norb * i
            ainv[half][i] = ainv[half][i] - wide_ref[at : at + norb, :]
    gorb_re, gorb_im = invert(*ainv)
    return gorb_re + gorb_im


def dress_kernel(norb, chips, freqs, own_ref, wide_ref, sum_ref, mat_ref):
    for k, row in enumerate(own_sum(norb, chips, freqs, 0, own_ref, wide_ref, mat_ref)):
        sum_ref[norb * k : norb * (k + 1), :] = row


def dyson_kernel(
    norb, chips, freqs, points, sib_ref, wide_ref, sum_ref, tile_ref, mat_ref, turn_ref
):
    pairs = norb * norb
    group = 2 * freqs

    def rows(ref, base):
        return [ref[base + norb * i : base + norb * (i + 1), :] for i in range(norb)]

    sig_re, sig_im = rows(wide_ref, 0), rows(wide_ref, pairs)
    sums = own_sum(norb, chips, freqs, 1, sib_ref, wide_ref, mat_ref)
    sums = [a + sum_ref[norb * k : norb * (k + 1), :] for k, a in enumerate(sums)]
    shift = chips // 2
    while shift:
        sums = [a + pltpu.roll(a, LANES - shift, 1) for a in sums]
        shift //= 2
    sums = [a * (1.0 / points) for a in sums]
    inv = invert(sums[:norb], sums[norb:])
    imp = rows(wide_ref, 2 * pairs), rows(wide_ref, 3 * pairs)
    pitch = turn_ref.shape[1] // norb
    diff = [[v - m for v, m in zip(inv[half], imp[half])] for half in range(2)]
    for half in range(2):
        for i in range(norb):
            turn_ref[half, pitch * i : pitch * i + norb, :] = diff[half][i]
    mat_ref[...] = jnp.zeros_like(mat_ref)
    for half, sig, sign in ((0, sig_re, 1.0), (1, sig_im, -1.0)):
        for i in range(norb):
            across = turn_ref[half, pl.ds(i, norb, stride=pitch), :]
            fresh = sig[i] + 0.5 * (diff[half][i] + sign * across)
            mat_ref[half, norb * i : norb * (i + 1), :] = fresh
    lines = []
    for half in range(2):
        flipped = mat_ref[half].T
        lines += [flipped[chips * f : chips * f + 1] for f in range(freqs)]
    lines = pack(lines, norb)
    for r, line in enumerate(lines):
        tile_ref[pl.ds(r, chips, stride=len(lines)), :] = jnp.broadcast_to(line, (chips, LANES))


def numbers_down(shape, chips, freqs, core):
    row = iota(shape, 0)
    part = row // LANES
    within = row - LANES * part
    place = within // chips
    return 2 * freqs * (within - chips * place) + freqs * (core ^ part) + place


def numbers(shape, chips, freqs, core):
    lane = iota(shape, 1)
    part = lane // LANES
    within = lane - LANES * part
    place = within // chips
    return 2 * freqs * (within - chips * place) + freqs * (core ^ part) + place


STEP = 16


def prepare_kernel(
    norb, chips, freqs, core_axis, energy_in, proj_in, window_in, sigma_ref, imp_ref, plain_ref,
    ainv_ref, green_ref, left_ref, side_ref, right_ref, wide_ref,
    energy_ref, proj_ref, window_ref, flat_ref, small_ref, sems,
):
    wait = fetched((energy_in, proj_in, window_in), (energy_ref, proj_ref, window_ref), sems)
    core = lax.axis_index(core_axis)
    pairs = norb * norb
    for which, ref in enumerate((sigma_ref, imp_ref)):
        for half in range(2):
            for i in range(norb):
                at = (which * 2 + half) * pairs + norb * i
                small_ref[at : at + norb, :] = ref[half, i]
    spread = jnp.where(iota((freqs, LANES), 1) // chips == iota((freqs, LANES), 0), 1.0, 0.0)
    wide_ref[...] = dot(small_ref[...], spread, NN)
    bands = energy_ref.shape[1]
    tall = green_ref.shape[1]
    count = green_ref.shape[2]
    rows = freqs * chips
    for part in range(2):
        mat = []
        for half in range(2):
            at = rows * (2 * part + half)
            turned = plain_ref[at : at + rows, :].T
            mat.append(rows_of(turned, norb))
        inv = invert(*mat)
        for half in range(2):
            for i in range(norb):
                ainv_ref[2 * half + part, norb * i : norb * (i + 1), :] = inv[half][i]

    flat_ref[...] = jnp.zeros_like(flat_ref)
    wait()
    for i in range(norb):
        flat_ref[i : i + 1, :bands] = proj_ref[0, i, 0:1]
        flat_ref[STEP + i : STEP + i + 1, :bands] = proj_ref[0, i, 1:2]
    flat_ref[2 * STEP : 2 * STEP + 1, :bands] = energy_ref[...]
    keep = band_inside(flat_ref.shape, window_ref) | (iota(flat_ref.shape, 0) >= 2 * STEP)
    turned = jnp.where(keep, flat_ref[...], 0.0).T[:tall]
    energy = turned[:, 2 * STEP : 2 * STEP + 1]
    freq = matsubara(numbers((tall, count), chips, freqs, core))
    denom = 1.0 / (energy * energy + freq * freq)
    green_re = -energy * denom
    green_im = -freq * denom
    green_ref[0] = green_re
    green_ref[1] = green_im
    wide = 2 * STEP
    straight = turned[:, :wide]
    high, low = split(straight)
    left_ref[...] = jnp.concatenate([high, high, low], axis=1)
    flat = jnp.where(keep, flat_ref[...], 0.0)
    span = flat.shape[1]
    energy = flat[2 * STEP : 2 * STEP + 1]
    freq = matsubara(numbers_down((count, span), chips, freqs, core))
    denom = 1.0 / (energy * energy + freq * freq)
    green_re = -energy * denom
    green_im = -freq * denom
    re, im = split(green_re), split(green_im)
    for k in range(2):
        right_ref[k, :, :span] = re[k]
        right_ref[k, :, span:] = im[k]
    side_ref[...] = jnp.zeros_like(side_ref)
    side_ref[:norb, :span] = flat[:norb]
    side_ref[:norb, span:] = flat[STEP : STEP + norb]


def solve(mat, rhs):
    size = len(mat[0])
    mat = [list(m) for m in mat]
    out = [list(r) for r in rhs]
    row = iota(mat[0][0].shape, 0)
    for p in range(size):
        at = row == p
        piv_re = mat[0][p][p : p + 1]
        piv_im = mat[1][p][p : p + 1]
        rec = 1.0 / (piv_re * piv_re + piv_im * piv_im)
        rec_re = piv_re * rec
        rec_im = -piv_im * rec
        old_re = jnp.where(at, -1.0, mat[0][p])
        old_im = jnp.where(at, 0.0, mat[1][p])
        col_re = old_re * rec_re - old_im * rec_im
        col_im = old_re * rec_im + old_im * rec_re
        for cols, start in ((mat, p + 1), (out, 0)):
            for q in range(start, size):
                x_re = cols[0][q][p : p + 1]
                x_im = cols[1][q][p : p + 1]
                rest_re = jnp.where(at, 0.0, cols[0][q])
                rest_im = jnp.where(at, 0.0, cols[1][q])
                cols[0][q] = rest_re - (col_re * x_re - col_im * x_im)
                cols[1][q] = rest_im - (col_re * x_im + col_im * x_re)
    return out


def vertex_part(norb, chips, freqs, core_axis, which, ref, ainv_ref, vert_ref, end_ref, sig_ref):
    core = lax.axis_index(core_axis)
    group = 2 * freqs
    lines = spaced(ref, chips, norb, group)
    for half in range(2):
        sig_ref[half] = upright(lines[freqs * half : freqs * (half + 1)])

    def columns(ref, first):
        return [ref[first, pl.ds(j, norb, stride=norb), :] for j in range(norb)]

    sig = [columns(sig_ref, half) for half in range(2)]
    mat = [
        [a - s for a, s in zip(columns(ainv_ref, 2 * half + which), sig[half])] for half in range(2)
    ]
    turned = solve(mat, sig)
    vert_ref[...] = jnp.zeros_like(vert_ref)
    for j in range(norb):
        sum_re, sum_im = sig[0][j], sig[1][j]
        for k in range(norb):
            y_re = turned[0][j][k : k + 1]
            y_im = turned[1][j][k : k + 1]
            sum_re = sum_re + (sig[0][k] * y_re - sig[1][k] * y_im)
            sum_im = sum_im + (sig[0][k] * y_im + sig[1][k] * y_re)
        at = 2 * LANES * j
        vert_ref[0:norb, at : at + LANES] = sum_re
        vert_ref[STEP : STEP + norb, at : at + LANES] = sum_im
        at += LANES
        vert_ref[0:norb, at : at + LANES] = sum_im
        vert_ref[STEP : STEP + norb, at : at + LANES] = -sum_re
    number = numbers((norb, 2 * LANES), chips, freqs, core)[:, LANES * which : LANES * (which + 1)]
    last = number == 2 * freqs * chips - 1
    orb = iota((norb, LANES), 1)
    end_ref[...] = jnp.zeros_like(end_ref)
    for half in range(2):
        end = jnp.zeros((norb, LANES), jnp.float32)
        for j in range(norb):
            entry = jnp.where(last, sig[half][j], 0.0)
            end = jnp.where(orb == j, jnp.sum(entry, axis=1, keepdims=True), end)
        end_ref[STEP * half : STEP * half + norb, :LANES] = end
        at = STEP * (1 - half)
        end_ref[at : at + norb, LANES:] = -end if half == 0 else end


def vertex_kernel(norb, chips, freqs, core_axis, own_ref, ainv_ref, vert_ref, end_ref, sig_ref):
    vertex_part(norb, chips, freqs, core_axis, 0, own_ref, ainv_ref, vert_ref, end_ref, sig_ref)


def density_kernel(
    norb, chips, freqs, core_axis, ainv_ref, green_ref, left_ref, side_ref, right_ref,
    first_ref, start_ref, tile_ref, sib_ref, out_ref, new_ref, sig_ref, vert_ref, end_ref, sums_ref,
):
    group = 2 * freqs
    kept = kept_rows(norb, group)
    tile = jnp.concatenate(unpack([tile_ref[k : k + 1, :] for k in range(kept)], norb, group), axis=0)
    for half in range(2):
        for i in range(norb):
            new_ref[half, i] = tile[freqs * half : freqs * (half + 1), norb * i : norb * (i + 1)]
    bands = out_ref.shape[2]
    tall = green_ref.shape[1]
    count = green_ref.shape[2]
    vertex_part(norb, chips, freqs, core_axis, 1, sib_ref, ainv_ref, vert_ref, end_ref, sig_ref)
    left = left_ref[...]

    def mixed(block):
        high, low = split(block)
        stacked = jnp.concatenate([high, low, high], axis=0)
        return lax.dot_general(left, stacked, NN, preferred_element_type=jnp.float32)

    def doubled(halves):
        size = halves[0].shape[1] // 2
        turned = [jnp.concatenate([-h[:, size:], h[:, :size]], axis=1) for h in halves]
        return [jnp.concatenate([a, b], axis=0) for a, b in zip(halves, turned)]

    def join(re, im, right):
        left = [jnp.concatenate([r, i], axis=1) for r, i in zip(split(re), split(im))]
        return dot3(left, right, NN)

    weight = -0.5 * inverse_temp * tail_weight(count)
    tail = weight * mixed(start_ref[...] + end_ref[...])
    total = join(tail[:, :LANES], tail[:, LANES:], doubled(split(side_ref[...])))
    span = sums_ref.shape[1]
    total_re, total_im = total[:, :span], total[:, span:]
    right_re = [right_ref[k, :, :span] for k in range(2)]
    right_im = [right_ref[k, :, span:] for k in range(2)]
    right_sum = split(
        (right_re[0].astype(jnp.float32) + right_im[0].astype(jnp.float32))
        + (right_re[1].astype(jnp.float32) + right_im[1].astype(jnp.float32))
    )
    green_re, green_im = green_ref[0], green_ref[1]
    for j in range(norb):
        block = []
        for half in range(2):
            at = LANES * (2 * j + half)
            block += [first_ref[:, at : at + LANES], vert_ref[:, at : at + LANES]]
        mix = mixed(jnp.concatenate(block, axis=1))
        mix_re, mix_im = mix[:, :count], mix[:, count:]
        side_re = mix_re * green_re - mix_im * green_im
        side_im = mix_re * green_im + mix_im * green_re
        prod_re = dot3(split(side_re), right_re, NN)
        prod_im = dot3(split(side_im), right_im, NN)
        prod_sum = dot3(split(side_re + side_im), right_sum, NN)
        both_re = prod_re - prod_im
        both_im = prod_sum - prod_re - prod_im
        p_re = side_ref[j : j + 1, :span]
        p_im = side_ref[j : j + 1, span:]
        total_re = total_re + (both_re * p_re - both_im * p_im)
        total_im = total_im + (both_re * p_im + both_im * p_re)
    sums_ref[...] = jnp.zeros_like(sums_ref)
    for half, total, sign in ((0, total_re, 1.0), (1, total_im, -1.0)):
        sums_ref[:tall, :] = total
        both = sums_ref[...] + sign * sums_ref[...].T
        out_ref[0, half] = both[:bands, :bands] / inverse_temp


HBM = pl.BlockSpec(memory_space=pltpu.HBM)
VMEM = pl.BlockSpec(memory_space=pltpu.VMEM)


def struct(*shape, dtype=jnp.float32):
    return jax.ShapeDtypeStruct(shape, dtype)


def scratch(*shape):
    return pltpu.VMEM(shape, jnp.float32)


def run(body, out, specs, scratches=()):
    return pl.pallas_call(
        body,
        out_shape=out,
        in_specs=specs,
        out_specs=jax.tree.map(lambda _: VMEM, out),
        scratch_shapes=scratches,
        compiler_params=pltpu.CompilerParams(vmem_limit_bytes=32 * 1024 * 1024),
    )


def kernels(norb, bands, freqs, chips, cores, points):
    group = 2 * freqs
    pairs = norb * norb
    count = freqs * chips * cores
    wide = -(-bands // LANES) * LANES
    tall = -(-bands // 16) * 16
    long = kept_rows(norb, 2 * group)
    short = kept_rows(norb, group)
    axis = "core"

    def project(*refs):
        project_kernel(norb, chips, freqs, axis, *refs)

    def dyson(*refs):
        dyson_kernel(norb, chips, freqs, points, *refs)

    def prepare(*refs):
        prepare_kernel(norb, chips, freqs, axis, *refs)

    def dress(*refs):
        dress_kernel(norb, chips, freqs, *refs)

    def vertex(*refs):
        vertex_kernel(norb, chips, freqs, axis, *refs)

    def rebuild(*refs):
        density_kernel(norb, chips, freqs, axis, *refs)

    inputs = [
        pltpu.VMEM((1, bands), jnp.float32),
        pltpu.VMEM((1, norb, 2, bands), jnp.float32),
        pltpu.VMEM((1, 2), jnp.int32),
    ]
    first = run(
        project,
        (struct(chips * long, LANES), struct(2 * count, LANES)),
        [HBM] * 3,
        [*inputs, scratch(32, wide), pltpu.SemaphoreType.DMA((3,))],
    )
    second = run(
        dyson,
        struct(chips * short, LANES),
        [VMEM] * 3,
        [scratch(2, LANES, LANES), scratch(2, 16 * norb, LANES)],
    )
    before = run(dress, struct(2 * pairs, LANES), [VMEM] * 2, [scratch(2, LANES, LANES)])
    after = run(
        vertex,
        (struct(2 * STEP, 2 * norb * LANES), struct(2 * STEP, 2 * LANES)),
        [VMEM] * 2,
        [scratch(2, LANES, LANES)],
    )
    aside = run(
        prepare,
        (
            struct(4, pairs, LANES),
            struct(2, tall, count),
            struct(tall, 6 * STEP, dtype=jnp.bfloat16),
            struct(LANES, 2 * wide),
            struct(2, count, 2 * wide, dtype=jnp.bfloat16),
            struct(4 * pairs, LANES),
        ),
        [HBM] * 3 + [VMEM] * 3,
        [
            *inputs,
            scratch(LANES, wide),
            scratch(4 * pairs, freqs),
            pltpu.SemaphoreType.DMA((3,)),
        ],
    )
    third = run(
        rebuild,
        (struct(1, 2, bands, bands), struct(2, norb, freqs, norb)),
        [VMEM] * 9,
        [
            scratch(2, LANES, LANES),
            scratch(2 * STEP, 2 * norb * LANES),
            scratch(2 * STEP, 2 * LANES),
            scratch(wide, wide),
        ],
    )
    return first, aside, before, second, after, third


def local(energies, proj, window, sigma, impurity_inverse):
    norb, bands = proj.shape[2:]
    freqs = sigma.shape[3]
    chips = lax.axis_size("z")
    cores = lax.axis_size("core")
    points = energies.shape[0] * chips * cores
    first, aside, before, second, after, third = kernels(norb, bands, freqs, chips, cores, points)
    swap = [(0, 1), (1, 0)]
    proj = jnp.swapaxes(proj, 1, 2)

    def across(rows):
        got = lax.all_to_all(rows.reshape(chips, 1, -1), "z", 0, 0, tiled=True)
        return got.reshape(rows.shape)

    far = [pltpu.with_memory_space_constraint(x, pltpu.HBM) for x in (energies, proj, window)]
    packed, plain = first(*far)
    ready = aside(*far, sigma, impurity_inverse, plain)
    got, ready = lax.optimization_barrier((across(packed), ready))
    *ready, spread = ready
    sibling = lax.ppermute(got, "core", swap)
    tiles = second(sibling, spread, before(got, spread))
    back = across(tiles)
    sibling = lax.ppermute(back, "core", swap)
    density, sigma_new = third(*ready, *after(back, ready[0]), tiles, sibling)
    return density, jnp.swapaxes(sigma_new, 2, 3)


def solution(mesh):
    parts, line = mesh.shape["parts"], mesh.shape["ka"]
    torus = Mesh(mesh.devices.reshape(parts, line // 2, 2), ("parts", "z", "core"))
    every = ("parts", "z", "core")
    line = ("z", "core")
    in_specs = (
        P(every, None),
        P(every, None, None, None),
        P(every, None),
        P("parts", None, None, line),
        P("parts", None, None, line),
    )
    out_specs = (P(every, None, None, None), P("parts", None, None, line))
    return jax.shard_map(local, mesh=torus, in_specs=in_specs, out_specs=out_specs, check_vma=False)
```
